128 devices in a mesh: row: 16 (over y, z), col: 8 (over x, core).
Axes of the slice: x: 4, y: 4, z: 4, core: 2. Of those that a mesh axis runs over, the one named last changes fastest.
Arguments:
- lower_panel: float32 [1, 4, 512, 8192], P(None, None, 'col', 'row'), may hold values from -4 to 4, as said below
- right_side: float32 [1, 8192, 8192], P(None, 'row', 'col'), may hold values from -6 to 6
Outputs:
- solution: float32 [4, 512, 8192], P(None, None, 'col')
- updated_rhs: float32 [1, 8192, 8192], P(None, 'row', 'col')
The draws below stay inside these ranges and needn't reach their ends.
Inputs may be any that keep to these rules, and one draw needn't show every extreme that they name: `lower_panel`: L is lower triangular: entries of tiles L[g, s] with g < s and above the diagonal of L[s, s] are zero; the diagonal entries of L lie between 2 and 4.
All inputs are finite; a program needn't handle non-finite values.
Results may differ from the reference program's by a relative error of at most 0.00017.
Values sent between devices are 32-bit elements; how exact they have to be, the bound alone decides.
A program may use at most 128 MiB of HBM per device.

```python
import jax
import jax.numpy as jnp
from jax import lax

NB = 512
STEPS = 4
ROUNDS = 1
R = 8192
N_ROW = 16


def draw_lower_panel(key, part):
    first_key, second_key = jax.random.split(jax.random.fold_in(key, 11), 2)
    shape = (ROUNDS, STEPS, NB, N_ROW * NB)
    base = jax.random.truncated_normal(first_key, -4.0, 4.0, shape, jnp.float32)
    diag_values = jax.random.uniform(second_key, shape, jnp.float32, 2.0, 4.0)
    round_idx = jnp.arange(ROUNDS, dtype=jnp.int32)[:, None, None, None]
    section_idx = jnp.arange(STEPS, dtype=jnp.int32)[None, :, None, None]
    column_idx = jnp.arange(NB, dtype=jnp.int32)[None, None, :, None]
    row_pos = jnp.arange(N_ROW * NB, dtype=jnp.int32)[None, None, None, :]
    tile_idx = round_idx * N_ROW + row_pos // NB
    inner_row = row_pos % NB
    below = base * (1.0 / (STEPS * NB) ** 0.5)
    inside = jnp.where(column_idx < inner_row, base * (3.0 / NB ** 0.5), jnp.where(column_idx == inner_row, diag_values, 0.0))
    values = jnp.where(tile_idx > section_idx, below, jnp.where(tile_idx == section_idx, inside, 0.0))
    return values.astype(jnp.float32)


def level_of(stream_key, shape, pieces, low, top_value):
    factor_of = 1.0
    for axis_at, shards_of in pieces:
        draws = jax.random.uniform(jax.random.fold_in(jax.random.fold_in(stream_key, 6), axis_at), (shards_of,), jnp.float32, low / len(pieces), top_value / len(pieces))
        factor_of = factor_of * jnp.repeat(jnp.exp(draws), shape[axis_at] // shards_of).reshape((-1,) + (1,) * (len(shape) - 1 - axis_at))
    return factor_of


def bell_draw(key, shape, deviation, bound, shards=(), kind=jnp.bfloat16):
    values = deviation * jax.random.normal(key, shape, jnp.float32)
    if shards:
        values = values * level_of(key, shape, shards, -0.22, 0.18)
    return jnp.clip(values, -bound, bound).astype(kind)


def setup_inputs(seed: int = 0) -> dict:
    splits = jax.random.split(jax.random.key(seed), 3)
    return {
        "lower_panel": draw_lower_panel(jax.random.fold_in(splits[2], 71), 0),
        "right_side": bell_draw(splits[1], (ROUNDS, N_ROW * NB, R), 1.0, 6.0, ((1, 16), (2, 8)), jnp.float32),
    }


def reference(lower_panel, right_side):
    tile_count = ROUNDS * N_ROW
    rhs_tiles = right_side.reshape(tile_count, NB, right_side.shape[2])
    low_blocks = lower_panel.reshape(ROUNDS, STEPS, NB, N_ROW, NB).transpose(0, 3, 1, 4, 2).reshape(tile_count, STEPS, NB, NB)
    tile_index = jnp.arange(tile_count, dtype=jnp.int32)
    solved_list = []
    for section in range(STEPS):
        solved = lax.linalg.triangular_solve(low_blocks[section, section], rhs_tiles[section], left_side=True, lower=True)
        update = jnp.einsum('gic,cx->gix', low_blocks[:, section], solved, precision=lax.Precision.HIGHEST)
        rhs_tiles = rhs_tiles - jnp.where((tile_index > section)[:, None, None], update, jnp.float32(0.0))
        solved_list.append(solved)
    return (jnp.stack(solved_list), rhs_tiles.reshape(ROUNDS, N_ROW * NB, right_side.shape[2]))
```

```python
import functools

import jax
import jax.numpy as jnp
from jax import lax
from jax.experimental import pallas as pl
from jax.experimental.pallas import tpu as pltpu
from jax.sharding import PartitionSpec as P

MESH = pl.DeviceIdType.MESH
NB = 512
CW = 128
A_CHUNKS = (0, 2, 3, 5, 7)
D_CHUNKS = (1, 4, 6)
N_SEND = 260
F32, BF16 = jnp.float32, jnp.bfloat16


def when(cond, fn):
    if cond is None:
        fn()
    else:
        pl.when(cond)(fn)


def gather_kernel(lp, b, g, ll, lo, own_sem, ga, gd, sl, sx, st, ox, ot, send):
    row, col = lax.axis_index("row"), lax.axis_index("col")
    y, z = row // 4, row % 4
    x, core = col // 2, col % 2

    def y_dev(d):
        return ((y + d + 4) % 4 * 4 + z, col)

    def z_dev(d):
        return (y * 4 + (z + d + 4) % 4, col)

    def x_dev(d):
        return (row, (x + d + 4) % 4 * 2 + core)

    partner = (row, x * 2 + 1 - core)
    blocks = [(z + d) % 4 for d in (0, 3, 1, 2)]
    OWN, LEFT, RIGHT, OPP = range(4)
    ops, sends = [], []

    def at(time, fn):
        ops.append((time, len(ops), fn))

    def put(src, dst, sem, dev, cond=None):
        slot = len(sends)

        def make():
            return pltpu.make_async_remote_copy(
                src_ref=src, dst_ref=dst, send_sem=send.at[slot], recv_sem=sem,
                device_id=dev, device_id_type=MESH,
            )

        sends.append((cond, make))
        when(cond, lambda: make().start())

    def got(ref, sem, cond=None):
        def body():
            pltpu.make_async_copy(ref, ref, sem).wait()

        when(cond, body)

    barrier = pltpu.get_barrier_semaphore()
    around = [y_dev(1), y_dev(-1), y_dev(2), z_dev(1), z_dev(-1), x_dev(1), x_dev(-1), partner]
    for dev in around:
        pl.semaphore_signal(barrier, inc=1, device_id=dev, device_id_type=MESH)

    root, other = y == 0, y != 0

    def l_ref(blk, k, j=None):
        return ll.at[blk, blk - k, col if j is None else j]

    def a_ref(blk, c):
        return g.at[blk, :, pl.ds(c * CW, CW)]

    def d_rows(q):
        return pl.ds(pl.multiple_of(q * 128, 128), 128)

    def d_ref(blk, c, q):
        return g.at[blk, d_rows(q), pl.ds(c * CW, CW)]

    for k in range(4):
        when(root & (z >= k), lambda k=k: pltpu.make_async_copy(lp.at[z - k], l_ref(z, k), sl.at[z, k]).start())
    for c in range(8):
        cols = pl.ds(c * CW, CW)
        if c in A_CHUNKS:
            when(root, lambda c=c, cols=cols: pltpu.make_async_copy(b.at[:, cols], a_ref(z, c), ga.at[z, c]).start())
        else:
            when(root, lambda c=c, cols=cols: pltpu.make_async_copy(
                b.at[pl.ds(0, 128), cols], d_ref(z, c, 0), gd.at[z, c, 0]).start())
    own_copies = [pltpu.make_async_copy(lp, lo.at[:, col], own_sem)]
    for cp in own_copies:
        cp.start()

    pl.semaphore_wait(barrier, len(around))

    def x_group(ref_of, xs, ts, cond, parity, t_send, t_fwd, t_last, src=None):
        xl, xr, xo = (x + 3) % 4, (x + 1) % 4, (x + 2) % 4

        def j_of(xx, cc):
            return xx * 2 + cc

        def start():
            s = ref_of(col) if src is None else src
            d = ref_of(col)
            put(s, d, xs.at[x], x_dev(1), cond)
            put(s, d, xs.at[x], x_dev(-1), cond)
            put(s, d, ts.at[x], partner, cond)

        def forward():
            for xx, here in ((xl, parity == 0), (xr, parity == 1)):
                r = ref_of(j_of(xx, core))
                got(r, xs.at[xx], cond)
                if here:
                    put(r, r, xs.at[xx], x_dev(1 if parity == 0 else -1), cond)
                put(r, r, ts.at[xx], partner, cond)

        def last():
            r = ref_of(j_of(xo, core))
            got(r, xs.at[xo], cond)
            put(r, r, ts.at[xo], partner, cond)

        def done():
            for xx in range(4):
                r = ref_of(j_of(xx, 1 - core))
                got(r, ts.at[xx], cond)

        at(t_send, start)
        at(t_fwd, forward)
        at(t_last, last)
        at(1000.0, done)

    for k in range(4):
        conds = [None if k == 0 else blk >= k for blk in blocks]

        def l_stage0(k=k, conds=conds):
            blk, cond = blocks[OWN], conds[OWN]
            r = l_ref(blk, k)
            got(r, sl.at[blk, k], cond)
            plus = k % 2 == 0
            go = (y != 3) if plus else (y != 1)
            put(r, r, sl.at[blk, k], y_dev(1 if plus else -1), go if cond is None else go & cond)
            put(r, r, sl.at[blk, k], z_dev(1), cond)
            put(r, r, sl.at[blk, k], z_dev(-1), cond)

        def l_stage1(k=k, conds=conds):
            for w in (LEFT, RIGHT):
                blk, cond = blocks[w], conds[w]
                r = l_ref(blk, k)
                got(r, sl.at[blk, k], cond)
                if (k % 2 == 0) == (w == LEFT):
                    put(r, r, sl.at[blk, k], z_dev(1 if w == LEFT else -1), cond)

        def l_stage2(k=k, conds=conds):
            blk, cond = blocks[OPP], conds[OPP]
            got(l_ref(blk, k), sl.at[blk, k], cond)

        at(2.0 + 2 * k, l_stage0)
        at(5.0 + 2 * k, l_stage1)
        at(8.0 + 2 * k, l_stage2)
        ready = (2.1 + 2 * k, 5.1 + 2 * k, 5.2 + 2 * k, 8.1 + 2 * k)
        for w in range(4):
            i = 4 * k + w
            x_group(
                lambda j, blk=blocks[w], k=k: l_ref(blk, k, j), sx.at[blocks[w], k], st.at[blocks[w], k],
                conds[w], i % 2, ready[w], 9.0 + 2.7 * i, 14.0 + 2.7 * i,
            )
    for h in range(2):
        def o_ref(j, h=h):
            return lo.at[pl.ds(2 * h, 2), j]

        x_group(o_ref, ox.at[h], ot.at[h], None, h, 12.0 + h, 46.0 + 3 * h, 52.0 + 3 * h,
                src=lp.at[pl.ds(2 * h, 2)])

    order = (0, 1, 2, 3, 4, 5, 6, 7)
    for i, c in enumerate(order):
        t = 5.0 + 6.0 * i
        if c in A_CHUNKS:
            n = A_CHUNKS.index(c)

            def a_stage0(c=c, n=n):
                r = a_ref(z, c)
                got(r, ga.at[z, c])
                plus = n % 2 == 0
                put(r, r, ga.at[z, c], y_dev(1 if plus else -1), (y != 3) if plus else (y != 1))
                put(r, r, ga.at[z, c], z_dev(1))
                put(r, r, ga.at[z, c], z_dev(-1))

            def a_stage1(c=c, n=n):
                for w in (LEFT, RIGHT):
                    blk = blocks[w]
                    r = a_ref(blk, c)
                    got(r, ga.at[blk, c])
                    if (n % 2 == 0) == (w == LEFT):
                        put(r, r, ga.at[blk, c], z_dev(1 if w == LEFT else -1))

            def a_stage2(c=c):
                blk = blocks[OPP]
                got(a_ref(blk, c), ga.at[blk, c])

            at(t, a_stage0)
            at(t + 7, a_stage1)
            at(t + 100, a_stage2)
        else:
            n = D_CHUNKS.index(c)

            def d_scatter(c=c):
                for q in (1, 3, 2):
                    put(b.at[pl.ds(q * 128, 128), pl.ds(c * CW, CW)], d_ref(z, c, q), gd.at[z, c, q], y_dev(q), root)

            def d_y(w, c=c):
                blk = blocks[w]
                r = d_ref(blk, c, y)
                put(r, r, gd.at[blk, c, y], y_dev(1))
                put(r, r, gd.at[blk, c, y], y_dev(-1))

            def d_stage0(c=c, d_y=d_y):
                r = d_ref(z, c, y)
                got(r, gd.at[z, c, y])
                put(r, r, gd.at[z, c, y], z_dev(1))
                put(r, r, gd.at[z, c, y], z_dev(-1))
                d_y(OWN)

            def d_stage1(c=c, n=n, d_y=d_y):
                for w in (LEFT, RIGHT):
                    blk = blocks[w]
                    r = d_ref(blk, c, y)
                    got(r, gd.at[blk, c, y])
                    if (n % 2 == 0) == (w == LEFT):
                        put(r, r, gd.at[blk, c, y], z_dev(1 if w == LEFT else -1))
                    d_y(w)

            def d_stage2(c=c, d_y=d_y):
                blk = blocks[OPP]
                got(d_ref(blk, c, y), gd.at[blk, c, y])
                d_y(OPP)

            def d_fwd(w, c=c):
                blk = blocks[w]
                for d in (-1, 1):
                    q = (y + d + 4) % 4
                    r = d_ref(blk, c, q)
                    got(r, gd.at[blk, c, q])
                    if (w % 2 == 0) == (d == -1):
                        put(r, r, gd.at[blk, c, q], y_dev(-d))

            def d_end(c=c):
                for blk in blocks:
                    q = (y + 2) % 4
                    got(d_ref(blk, c, q), gd.at[blk, c, q])

            at(1.0 + 0.1 * i if i < 2 else t - 8, d_scatter)
            at(t, d_stage0)
            at(t + 4, d_stage1)
            at(t + 7, d_stage2)
            at(t + 5, functools.partial(d_fwd, OWN))
            at(t + 9, functools.partial(d_fwd, LEFT))
            at(t + 9.1, functools.partial(d_fwd, RIGHT))
            at(t + 12, functools.partial(d_fwd, OPP))
            at(t + 100, d_end)

    for _, _, fn in sorted(ops, key=lambda o: o[:2]):
        fn()
    for cond, make in sends:
        when(cond, lambda make=make: make().wait_send())
    for cp in own_copies:
        cp.wait()


def dot(a, b):
    return jnp.dot(a, b, preferred_element_type=F32)


def exact(a, b):
    return jnp.dot(a, b, preferred_element_type=F32, precision=lax.Precision.HIGHEST)


def split(v):
    hi = v.astype(BF16)
    return hi, (v - hi.astype(F32)).astype(BF16)


def invert_tiles(tiles):
    n = 128
    ri = lax.broadcasted_iota(jnp.int32, (n, n), 0)
    ci = lax.broadcasted_iota(jnp.int32, (n, n), 1)
    eye = ri == ci
    ident = jnp.where(eye, F32(1.0), F32(0.0))
    count = len(tiles)
    scaled, inv_row, parts = [], [], []
    for t in tiles:
        cols, rows = [], []
        for d in range(4):
            blk = t[d * n:(d + 1) * n, d * n:(d + 1) * n]
            diag = jnp.where(eye, blk, F32(0.0))
            cols.append(F32(1.0) / jnp.sum(diag, axis=1, keepdims=True))
            rows.append(F32(1.0) / jnp.sum(diag, axis=0, keepdims=True))
        scaled.append(t * jnp.concatenate(cols, axis=0))
        inv_row.append(jnp.concatenate(rows, axis=1))
    for t in scaled:
        for d in range(4):
            parts.append(jnp.where(ri > ci, t[d * n:(d + 1) * n, d * n:(d + 1) * n], F32(0.0)))
    same8 = (ri // 8) == (ci // 8)
    small = [jnp.where(same8, p, F32(0.0)) for p in parts]
    sq = [exact(m, m) for m in small]
    inv = [(ident - m) for m in small]
    step = [exact(v, q) for v, q in zip(inv, sq)]
    quad = [exact(q, q) for q in sq]
    inv = [v + s for v, s in zip(inv, step)]
    step = [exact(v, q) for v, q in zip(inv, quad)]
    inv = [v + s for v, s in zip(inv, step)]
    for w in (8, 16, 32, 64):
        mask = (ri // (2 * w) == ci // (2 * w)) & ((ri // w) != (ci // w))
        low = [exact(jnp.where(mask, p, F32(0.0)), v) for p, v in zip(parts, inv)]
        step = [exact(v, s) for v, s in zip(inv, low)]
        inv = [v - s for v, s in zip(inv, step)]
    zero = jnp.zeros((n, n), F32)
    pairs = []
    low = []
    for k in range(count):
        for h in range(2):
            a, c = 2 * h, 2 * h + 1
            low.append(exact(scaled[k][c * n:(c + 1) * n, a * n:(a + 1) * n], inv[4 * k + a]))
    for k in range(count):
        for h in range(2):
            a, c = inv[4 * k + 2 * h], inv[4 * k + 2 * h + 1]
            e = -exact(c, low[2 * k + h])
            pairs.append(jnp.concatenate(
                [jnp.concatenate([a, zero], axis=1), jnp.concatenate([e, c], axis=1)], axis=0))
    low = [exact(scaled[k][256:, :256], pairs[2 * k]) for k in range(count)]
    zero = jnp.zeros((256, 256), F32)
    out = []
    for k in range(count):
        e = -exact(pairs[2 * k + 1], low[k])
        full = jnp.concatenate(
            [jnp.concatenate([pairs[2 * k], zero], axis=1), jnp.concatenate([e, pairs[2 * k + 1]], axis=1)], axis=0)
        out.append(full * inv_row[k])
    return out


def solve_kernel(g, ll, lo, b, x_out, c_out, lh, lw, vh, vw, oh, ow, xh, xw):
    row = lax.axis_index("row")

    @pl.when(pl.program_id(0) == 0)
    def _():
        for r in range(4):
            for s in range(r):
                cols = pl.ds(s * NB, NB)
                lh[r - 1, :, cols], lw[r - 1, :, cols] = split(ll[r, s].T)
        for s in range(4):
            cols = pl.ds(s * NB, NB)
            oh[:, cols], ow[:, cols] = split(jnp.where(row > s, lo[s], F32(0.0)).T)
        for s, v in enumerate(invert_tiles([ll[s, s].T for s in range(4)])):
            vh[s], vw[s] = split(v)

    for r in range(4):
        rhs = g[r]
        if r:
            k = pl.ds(0, r * NB)
            a, aw, v, vv = lh[r - 1, :, k], lw[r - 1, :, k], xh[k, :], xw[k, :]
            rhs = rhs - (dot(a, v) + (dot(a, vv) + dot(aw, v)))
        hi, low = split(rhs)
        out = dot(vh[r], hi) + (dot(vh[r], low) + dot(vw[r], hi))
        x_out[r] = out
        rows = pl.ds(r * NB, NB)
        xh[rows, :], xw[rows, :] = split(out)
    upd = dot(oh[...], xh[...]) + (dot(oh[...], xw[...]) + dot(ow[...], xh[...]))
    c_out[...] = b[...] - upd


def per_device(lower_panel, right_side):
    lp, b = lower_panel[0], right_side[0]
    width = b.shape[1]
    dma = pltpu.SemaphoreType.DMA
    hbm = pl.BlockSpec(memory_space=pl.ANY)
    g, ll, lo = pl.pallas_call(
        gather_kernel,
        out_shape=(
            jax.ShapeDtypeStruct((4, NB, width), F32),
            jax.ShapeDtypeStruct((4, 4, 8, 64, NB), F32),
            jax.ShapeDtypeStruct((4, 8, 64, NB), F32),
        ),
        in_specs=[hbm, hbm],
        out_specs=(hbm, hbm, hbm),
        scratch_shapes=[
            dma(()), dma((4, 8)), dma((4, 8, 4)), dma((4, 4)), dma((4, 4, 4)), dma((4, 4, 4)),
            dma((2, 4)), dma((2, 4)), dma((N_SEND,)),
        ],
        compiler_params=pltpu.CompilerParams(collective_id=0, has_side_effects=True),
        name="gather",
    )(lp, b)
    ll = ll.reshape(4, 4, NB, NB)
    lo = lo.reshape(4, NB, NB)
    w = 256
    vmem = pl.BlockSpec(memory_space=pltpu.VMEM)
    x, c = pl.pallas_call(
        solve_kernel,
        grid=(width // w,),
        out_shape=(jax.ShapeDtypeStruct((4, NB, width), F32), jax.ShapeDtypeStruct((NB, width), F32)),
        in_specs=[
            pl.BlockSpec((4, NB, w), lambda i: (0, 0, i)), vmem, vmem,
            pl.BlockSpec((NB, w), lambda i: (0, i)),
        ],
        out_specs=(pl.BlockSpec((4, NB, w), lambda i: (0, 0, i)), pl.BlockSpec((NB, w), lambda i: (0, i))),
        scratch_shapes=[
            pltpu.VMEM((3, NB, 3 * NB), BF16), pltpu.VMEM((3, NB, 3 * NB), BF16),
            pltpu.VMEM((4, NB, NB), BF16), pltpu.VMEM((4, NB, NB), BF16),
            pltpu.VMEM((NB, 4 * NB), BF16), pltpu.VMEM((NB, 4 * NB), BF16),
            pltpu.VMEM((4 * NB, w), BF16), pltpu.VMEM((4 * NB, w), BF16),
        ],
        compiler_params=pltpu.CompilerParams(vmem_limit_bytes=66_000_000),
        name="solve",
    )(g, ll, lo, b)
    return x, c[None]


def solution(mesh):
    return jax.shard_map(
        per_device,
        mesh=mesh,
        in_specs=(P(None, None, "col", "row"), P(None, "row", "col")),
        out_specs=(P(None, None, "col"), P(None, "row", "col")),
        check_vma=False,
    )
```

```python
import functools

import jax
import jax.numpy as jnp
from jax import lax
from jax.experimental import pallas as pl
from jax.experimental.pallas import tpu as pltpu
from jax.sharding import PartitionSpec as P

MESH = pl.DeviceIdType.MESH
NB = 512
CW = 128
Z_FIRST = (2, 5, 7)
N_SEND = 400
TIMES = (11, 17, 25, 29, 30, 38, 48, 75, 66, 83, 141, 190, 104, 157, 87, 119, 169, 112, 100, 185, 0, 1, 12, 7, 13, 28, 23, 36, 156, 130, 164, 40, 126, 93, 99, 43, 68, 61, 178, 122, 31, 39, 41, 51, 52, 74, 73, 84, 110, 64, 193, 123, 135, 161, 90, 133, 196, 121, 114, 150, 2, 3, 21, 8, 22, 49, 44, 71, 129, 80, 175, 142, 116, 170, 95, 155, 172, 105, 163, 138, 6, 32, 20, 62, 14, 117, 58, 146, 10, 109, 176, 139, 27, 82, 65, 97, 4, 9, 16, 19, 35, 63, 162, 188, 120, 45, 103, 127, 106, 5, 15, 47, 24, 76, 101, 181, 145, 115, 195, 60, 91, 191, 26, 34, 56, 50, 69, 140, 166, 152, 186, 57, 183, 111, 107, 18, 33, 37, 59, 128, 86, 85, 165, 154, 102, 77, 158, 174, 46, 55, 78, 89, 98, 113, 173, 182, 147, 180, 177, 192, 143, 42, 53, 70, 94, 124, 134, 72, 118, 149, 194, 144, 168, 131, 67, 81, 92, 96, 137, 151, 167, 179, 171, 197, 159, 198, 199, 54, 79, 108, 88, 125, 160, 148, 136, 132, 153, 187, 184, 189)
F32, BF16 = jnp.float32, jnp.bfloat16


def when(cond, fn):
    if cond is None:
        fn()
    else:
        pl.when(cond)(fn)


def gather_kernel(lp, b, g, ll, lo, own_sem, gs, sq, sl, sx, st, ox, ot, send):
    row, col = lax.axis_index("row"), lax.axis_index("col")
    y, z = row // 4, row % 4
    x, core = col // 2, col % 2

    def y_dev(d):
        return ((y + d + 4) % 4 * 4 + z, col)

    def z_dev(d):
        return (y * 4 + (z + d + 4) % 4, col)

    def x_dev(d):
        return (row, (x + d + 4) % 4 * 2 + core)

    partner = (row, x * 2 + 1 - core)
    blocks = [(z + d) % 4 for d in (0, 3, 1, 2)]
    OWN, LEFT, RIGHT, OPP = range(4)
    ops, ends, sends = [], [], []
    task, last = ops.append, ends.append

    def put(src, dst, sem, dev, cond=None):
        slot = len(sends)

        def make():
            return pltpu.make_async_remote_copy(
                src_ref=src, dst_ref=dst, send_sem=send.at[slot], recv_sem=sem,
                device_id=dev, device_id_type=MESH,
            )

        sends.append((cond, make))
        when(cond, lambda: make().start())

    def got(ref, sem, cond=None):
        def body():
            pltpu.make_async_copy(ref, ref, sem).wait()

        when(cond, body)

    barrier = pltpu.get_barrier_semaphore()
    around = [y_dev(1), y_dev(-1), y_dev(2), z_dev(1), z_dev(-1), x_dev(1), x_dev(-1), partner]
    for dev in around:
        pl.semaphore_signal(barrier, inc=1, device_id=dev, device_id_type=MESH)

    root, other = y == 0, y != 0

    def l_ref(blk, k, j=None):
        return ll.at[blk, blk - k, col if j is None else j]

    def piece(blk, c, q):
        return g.at[blk, pl.ds(pl.multiple_of(q * 128, 128), 128), pl.ds(c * CW, CW)]

    def l_quarter(k, q):
        return ll.at[z, z - k, col, pl.ds(pl.multiple_of(q * 16, 16), 16)]

    for k in range(4):
        when(root & (z >= k), lambda k=k: pltpu.make_async_copy(
            lp.at[z - k, pl.ds(0, 16)], l_quarter(k, 0), sq.at[k, 0]).start())
    for c in range(8):
        when(root, lambda c=c: pltpu.make_async_copy(
            b.at[pl.ds(0, 128), pl.ds(c * CW, CW)], piece(z, c, 0), gs.at[z, c, 0]).start())
    own_copies = [pltpu.make_async_copy(lp, lo.at[:, col], own_sem)]
    for cp in own_copies:
        cp.start()

    pl.semaphore_wait(barrier, len(around))

    def x_group(ref_of, xs, ts, cond, parity, src=None):
        def j_of(xx, cc):
            return xx * 2 + cc

        def start():
            s = ref_of(col) if src is None else src
            d = ref_of(col)
            put(s, d, xs.at[x], x_dev(1), cond)
            put(s, d, xs.at[x], x_dev(-1), cond)
            put(s, d, ts.at[x], partner, cond)

        def arrive(d, relay):
            xx = (x + d + 4) % 4
            r = ref_of(j_of(xx, core))
            got(r, xs.at[xx], cond)
            if relay:
                put(r, r, xs.at[xx], x_dev(-d), cond)
            put(r, r, ts.at[xx], partner, cond)

        def done():
            for xx in range(4):
                got(ref_of(j_of(xx, 1 - core)), ts.at[xx], cond)

        return start, arrive, done

    for k in range(4):
        conds = [None if k == 0 else blk >= k for blk in blocks]
        groups = [
            x_group(lambda j, blk=blocks[w], k=k: l_ref(blk, k, j), sx.at[blocks[w], k], st.at[blocks[w], k],
                    conds[w], (k + w) % 2)
            for w in range(4)
        ]

        def l_scatter(k=k, cond=conds[OWN]):
            for q in (1, 3, 2):
                put(lp.at[z - k, pl.ds(q * 16, 16)], l_quarter(k, q), sq.at[k, q], y_dev(q),
                    root if cond is None else root & cond)

        def l_mine(k=k, cond=conds[OWN]):
            r, sem = l_quarter(k, y), sq.at[k, y]
            got(r, sem, cond)
            put(r, r, sem, y_dev(1), cond)
            put(r, r, sem, y_dev(-1), cond)

        def l_relay(d, k=k, cond=conds[OWN]):
            q = (y + d + 4) % 4
            r, sem = l_quarter(k, q), sq.at[k, q]
            got(r, sem, cond)
            if d == (-1 if k % 2 == 0 else 1):
                put(r, r, sem, y_dev(-d), cond)

        def l_own(k=k, cond=conds[OWN], start=groups[OWN][0]):
            q = (y + 2) % 4
            got(l_quarter(k, q), sq.at[k, q], cond)
            r, sem = l_ref(z, k), sl.at[z, k]
            put(r, r, sem, z_dev(1), cond)
            put(r, r, sem, z_dev(-1), cond)
            start()

        def l_arrive(w, k=k, conds=conds, groups=groups):
            blk, cond = blocks[w], conds[w]
            r, sem = l_ref(blk, k), sl.at[blk, k]
            got(r, sem, cond)
            if w == (LEFT if k % 2 == 0 else RIGHT):
                put(r, r, sem, z_dev(1 if w == LEFT else -1), cond)
            groups[w][0]()

        task(l_scatter)
        task(l_mine)
        task(functools.partial(l_relay, -1))
        task(functools.partial(l_relay, 1))
        task(l_own)
        for w in (LEFT, RIGHT, OPP):
            task(functools.partial(l_arrive, w))
        for w in range(4):
            for d in (-1, 1, 2):
                task(functools.partial(groups[w][1], d, d == (-1 if (k + w) % 2 == 0 else 1)))
            last(groups[w][2])
    for h in range(4):
        start, arrive, done = x_group(lambda j, h=h: lo.at[h, j], ox.at[h], ot.at[h], None, h % 2, src=lp.at[h])
        task(start)
        for d in (-1, 1, 2):
            task(functools.partial(arrive, d, d == (-1 if h % 2 == 0 else 1)))
        last(done)

    for c in range(8):
        def scatter(c=c):
            for q in (1, 3, 2):
                put(b.at[pl.ds(q * 128, 128), pl.ds(c * CW, CW)], piece(z, c, q), gs.at[z, c, q], y_dev(q), root)

        zfirst = c in Z_FIRST
        pos1, pos2 = (z, y) if zfirst else (y, z)
        dev1, dev2 = (z_dev, y_dev) if zfirst else (y_dev, z_dev)

        def at(e, d, c=c, pos1=pos1, pos2=pos2, zfirst=zfirst):
            i1, i2 = (pos1 + e + 4) % 4, (pos2 + d + 4) % 4
            blk, q = (i1, i2) if zfirst else (i2, i1)
            return piece(blk, c, q), gs.at[blk, c, q]

        def first(e, c=c, at=at, dev1=dev1, dev2=dev2):
            r, sem = at(e, 0)
            got(r, sem)
            if e == 0:
                put(r, r, sem, dev1(1))
                put(r, r, sem, dev1(-1))
            elif e == (-1 if c // 2 % 2 == 0 else 1):
                put(r, r, sem, dev1(-e))
            put(r, r, sem, dev2(1))
            put(r, r, sem, dev2(-1))

        def second(e, d, at=at, dev2=dev2):
            r, sem = at(e, d)
            got(r, sem)
            if d == (-1 if e in (0, 2) else 1):
                put(r, r, sem, dev2(-d))

        task(scatter)
        for e in (0, -1, 1, 2):
            task(functools.partial(first, e))
        for e in (0, -1, 1, 2):
            for d in (-1, 1):
                task(functools.partial(second, e, d))
            last(functools.partial(second, e, 2))

    order = sorted(range(len(ops)), key=lambda i: (TIMES[i] if i < len(TIMES) else i, i))
    for i in order:
        ops[i]()
    for fn in ends:
        fn()
    for cond, make in sends:
        when(cond, lambda make=make: make().wait_send())
    for cp in own_copies:
        cp.wait()


def dot(a, b):
    return jnp.dot(a, b, preferred_element_type=F32)


def split(v):
    hi = v.astype(BF16)
    return hi, (v - hi.astype(F32)).astype(BF16)


def dot_small(a, b):
    bb = jnp.concatenate(split(b), axis=1)
    r = dot(jnp.concatenate(split(a), axis=1), jnp.concatenate([bb, bb], axis=0))
    return r[:, :128] + r[:, 128:]


def dot3(a, b):
    (ah, al), (bh, bl) = split(a), split(b)
    return dot(ah, bh) + (dot(ah, bl) + dot(al, bh))


def invert_tiles(tiles):
    n = 128
    ri = lax.broadcasted_iota(jnp.int32, (n, n), 0)
    ci = lax.broadcasted_iota(jnp.int32, (n, n), 1)
    eye = ri == ci
    ident = jnp.where(eye, F32(1.0), F32(0.0))
    count = len(tiles)
    scaled, inv_row, parts = [], [], []
    for t in tiles:
        cols, rows = [], []
        for d in range(4):
            blk = t[d * n:(d + 1) * n, d * n:(d + 1) * n]
            diag = jnp.where(eye, blk, F32(0.0))
            cols.append(F32(1.0) / jnp.sum(diag, axis=1, keepdims=True))
            rows.append(F32(1.0) / jnp.sum(diag, axis=0, keepdims=True))
        scaled.append([[t[a * n:(a + 1) * n, c * n:(c + 1) * n] * cols[a] for c in range(a + 1)] for a in range(4)])
        inv_row.append(jnp.concatenate(rows, axis=1))
    for t in scaled:
        for d in range(4):
            parts.append(jnp.where(ri > ci, t[d][d], F32(0.0)))
    same8 = (ri // 8) == (ci // 8)
    small = [jnp.where(same8, p, F32(0.0)) for p in parts]
    sq = [dot_small(m, m) for m in small]
    inv = [(ident - m) for m in small]
    step = [dot_small(v, q) for v, q in zip(inv, sq)]
    quad = [dot_small(q, q) for q in sq]
    inv = [v + s for v, s in zip(inv, step)]
    step = [dot_small(v, q) for v, q in zip(inv, quad)]
    inv = [v + s for v, s in zip(inv, step)]
    for w in (8, 16, 32, 64):
        mask = (ri // (2 * w) == ci // (2 * w)) & ((ri // w) != (ci // w))
        low = [dot_small(jnp.where(mask, p, F32(0.0)), v) for p, v in zip(parts, inv)]
        step = [dot_small(v, s) for v, s in zip(inv, low)]
        inv = [v - s for v, s in zip(inv, step)]
    zero = jnp.zeros((n, n), F32)
    pairs, low = [], []
    for k in range(count):
        for h in range(2):
            low.append(dot_small(scaled[k][2 * h + 1][2 * h], inv[4 * k + 2 * h]))
    for k in range(count):
        for h in range(2):
            a, c = inv[4 * k + 2 * h], inv[4 * k + 2 * h + 1]
            e = -dot_small(c, low[2 * k + h])
            pairs.append(jnp.concatenate(
                [jnp.concatenate([a, zero], axis=1), jnp.concatenate([e, c], axis=1)], axis=0))
    low = []
    for k in range(count):
        t = scaled[k]
        corner = jnp.concatenate(
            [jnp.concatenate(t[2][:2], axis=1), jnp.concatenate(t[3][:2], axis=1)], axis=0)
        low.append(dot3(corner, pairs[2 * k]))
    zero = jnp.zeros((256, 256), F32)
    out = []
    for k in range(count):
        e = -dot3(pairs[2 * k + 1], low[k])
        full = jnp.concatenate(
            [jnp.concatenate([pairs[2 * k], zero], axis=1), jnp.concatenate([e, pairs[2 * k + 1]], axis=1)], axis=0)
        out.append(full * inv_row[k])
    return out


STACK = (0, 2048, 3584, 4608, 5120)


def solve_kernel(g, ll, lo, b, x_out, c_out, tiles, sh, sw, vh, vw, acc, sems):
    row = lax.axis_index("row")

    @pl.when(pl.program_id(0) == 0)
    def _():
        wanted = [("d", s, s) for s in range(4)]
        wanted += [("l", r, s) for s in range(4) for r in range(s + 1, 4)]
        wanted += [("o", 0, s) for s in range(4)]
        copies = [
            pltpu.make_async_copy(lo.at[s] if kind == "o" else ll.at[r, s], tiles.at[n], sems.at[n])
            for n, (kind, r, s) in enumerate(wanted)
        ]
        for cp in copies:
            cp.start()
        for cp in copies[:4]:
            cp.wait()
        for s, v in enumerate(invert_tiles([tiles[s].T for s in range(4)])):
            vh[s], vw[s] = split(v)
        for n, (kind, r, s) in enumerate(wanted):
            if n < 4:
                continue
            copies[n].wait()
            t = tiles[n]
            if kind == "o":
                t = jnp.where(row > s, t, F32(0.0))
                rows = pl.ds(STACK[s + 1] - NB, NB)
            else:
                rows = pl.ds(STACK[s] + (r - s - 1) * NB, NB)
            sh[rows, :], sw[rows, :] = split(t.T)

    for s in range(4):
        hi, low = split(g[0] if s == 0 else acc[s - 1])
        x = dot(vh[s], hi) + (dot(vh[s], low) + dot(vw[s], hi))
        x_out[s] = x
        hi, low = split(x)
        rows = pl.ds(STACK[s], STACK[s + 1] - STACK[s])
        upd = dot(sh[rows, :], hi) + (dot(sh[rows, :], low) + dot(sw[rows, :], hi))
        for r in range(s + 1, 4):
            base = g[r] if s == 0 else acc[r - 1]
            acc[r - 1] = base - upd[(r - s - 1) * NB:(r - s) * NB]
        own = (b[...] if s == 0 else acc[3]) - upd[(3 - s) * NB:]
        if s == 3:
            c_out[...] = own
        else:
            acc[3] = own


def per_device(lower_panel, right_side):
    lp, b = lower_panel[0], right_side[0]
    width = b.shape[1]
    dma = pltpu.SemaphoreType.DMA
    hbm = pl.BlockSpec(memory_space=pl.ANY)
    g, ll, lo = pl.pallas_call(
        gather_kernel,
        out_shape=(
            jax.ShapeDtypeStruct((4, NB, width), F32),
            jax.ShapeDtypeStruct((4, 4, 8, 64, NB), F32),
            jax.ShapeDtypeStruct((4, 8, 64, NB), F32),
        ),
        in_specs=[hbm, hbm],
        out_specs=(hbm, hbm, hbm),
        scratch_shapes=[
            dma(()), dma((4, 8, 4)), dma((4, 4)), dma((4, 4)), dma((4, 4, 4)), dma((4, 4, 4)),
            dma((4, 4)), dma((4, 4)), dma((N_SEND,)),
        ],
        compiler_params=pltpu.CompilerParams(collective_id=0, has_side_effects=True),
        name="gather",
    )(lp, b)
    ll = ll.reshape(4, 4, NB, NB)
    lo = lo.reshape(4, NB, NB)
    w = 512
    x, c = pl.pallas_call(
        solve_kernel,
        grid=(width // w,),
        out_shape=(jax.ShapeDtypeStruct((4, NB, width), F32), jax.ShapeDtypeStruct((NB, width), F32)),
        in_specs=[
            pl.BlockSpec((4, NB, w), lambda i: (0, 0, i)), hbm, hbm,
            pl.BlockSpec((NB, w), lambda i: (0, i)),
        ],
        out_specs=(pl.BlockSpec((4, NB, w), lambda i: (0, 0, i)), pl.BlockSpec((NB, w), lambda i: (0, i))),
        scratch_shapes=[
            pltpu.VMEM((14, NB, NB), F32),
            pltpu.VMEM((STACK[4], NB), BF16), pltpu.VMEM((STACK[4], NB), BF16),
            pltpu.VMEM((4, NB, NB), BF16), pltpu.VMEM((4, NB, NB), BF16),
            pltpu.VMEM((4, NB, w), F32),
            dma((14,)),
        ],
        compiler_params=pltpu.CompilerParams(vmem_limit_bytes=66_000_000),
        name="solve",
    )(g, ll, lo, b)
    return x, c[None]


def solution(mesh):
    return jax.shard_map(
        per_device,
        mesh=mesh,
        in_specs=(P(None, None, "col", "row"), P(None, "row", "col")),
        out_specs=(P(None, None, "col"), P(None, "row", "col")),
        check_vma=False,
    )
```

```python
import functools

import jax
import jax.numpy as jnp
from jax import lax
from jax.experimental import pallas as pl
from jax.experimental.pallas import tpu as pltpu
from jax.sharding import PartitionSpec as P

MESH = pl.DeviceIdType.MESH
NB = 512
CW = 128
HALF = 512
Z_FIRST = (2, 5, 7)
N_SEND = 400
TIMES = (11, 19, 29, 45, 46, 65, 67, 96, 64, 102, 109, 99, 115, 137, 98, 95, 139, 108, 114, 120, 140, 159, 173, 163, 0, 1, 7, 9, 10, 28, 20, 49, 52, 34, 56, 50, 144, 84, 86, 107, 161, 135, 70, 197, 83, 149, 211, 215, 26, 38, 57, 55, 75, 101, 127, 122, 112, 145, 148, 130, 134, 184, 172, 191, 202, 178, 169, 182, 185, 205, 204, 200, 2, 12, 24, 13, 25, 60, 41, 72, 153, 71, 142, 103, 146, 183, 90, 78, 198, 104, 79, 143, 240, 227, 222, 203, 18, 224, 31, 252, 3, 147, 35, 221, 4, 21, 88, 51, 17, 230, 27, 164, 6, 16, 74, 37, 106, 151, 208, 218, 105, 76, 187, 133, 129, 237, 176, 225, 234, 5, 14, 36, 23, 111, 33, 42, 80, 119, 188, 47, 125, 201, 195, 196, 214, 162, 15, 30, 43, 59, 73, 62, 124, 68, 61, 116, 91, 110, 82, 97, 229, 156, 236, 8, 22, 32, 54, 87, 39, 92, 93, 66, 223, 121, 158, 226, 77, 138, 210, 193, 40, 48, 117, 58, 165, 155, 168, 160, 150, 132, 94, 219, 186, 255, 231, 128, 253, 63, 100, 113, 199, 131, 170, 167, 192, 154, 254, 232, 166, 257, 212, 179, 258, 213, 44, 69, 89, 81, 157, 175, 220, 190, 141, 194, 209, 207, 189, 228, 180, 251, 250, 53, 85, 136, 118, 152, 123, 171, 239, 177, 235, 126, 181, 217, 233, 249, 248, 256, 174, 216, 206, 241, 238, 242, 243, 244, 245, 246, 247, 267, 259, 260, 261, 262, 263, 264, 265, 266)
F32, BF16 = jnp.float32, jnp.bfloat16


def when(cond, fn):
    if cond is None:
        fn()
    else:
        pl.when(cond)(fn)


def arrange(meta, times):
    eff = [float(times[i]) if i < len(times) else float(i) for i in range(len(meta))]
    for i, (_, needs) in enumerate(meta):
        for j in range(i):
            if meta[j][0] in needs and eff[j] >= eff[i]:
                eff[i] = eff[j] + 1e-3
    return sorted(range(len(meta)), key=lambda i: (eff[i], i))


def gather_kernel(lp, b, x_out, lo, g, ll, xb, sh, sw, vh, vw, xh, xl, own_sem, gs, sq, sl, sx, st, ox, ot, send, osem):
    row, col = lax.axis_index("row"), lax.axis_index("col")
    y, z = row // 4, row % 4
    x, core = col // 2, col % 2

    def y_dev(d):
        return ((y + d + 4) % 4 * 4 + z, col)

    def z_dev(d):
        return (y * 4 + (z + d + 4) % 4, col)

    def x_dev(d):
        return (row, (x + d + 4) % 4 * 2 + core)

    partner = (row, x * 2 + 1 - core)
    blocks = [(z + d) % 4 for d in (0, 3, 1, 2)]
    OWN, LEFT, RIGHT, OPP = range(4)
    ops, meta, ends, sends = [], [], [], []
    last = ends.append

    def task(fn, tag=None, needs=()):
        ops.append(fn)
        meta.append((tag, needs))

    def put(src, dst, sem, dev, cond=None):
        slot = len(sends)

        def make():
            return pltpu.make_async_remote_copy(
                src_ref=src, dst_ref=dst, send_sem=send.at[slot], recv_sem=sem,
                device_id=dev, device_id_type=MESH,
            )

        sends.append((cond, make))
        when(cond, lambda: make().start())

    def got(ref, sem, cond=None):
        def body():
            pltpu.make_async_copy(ref, ref, sem).wait()

        when(cond, body)

    barrier = pltpu.get_barrier_semaphore()
    around = [y_dev(1), y_dev(-1), y_dev(2), z_dev(1), z_dev(-1), x_dev(1), x_dev(-1), partner]
    for dev in around:
        pl.semaphore_signal(barrier, inc=1, device_id=dev, device_id_type=MESH)

    root, other = y == 0, y != 0

    def l_ref(blk, k, j=None):
        return ll.at[blk * (blk + 1) // 2 + blk - k, col if j is None else j]

    def piece(blk, c, q):
        return g.at[blk, pl.ds(pl.multiple_of(q * 128, 128), 128), pl.ds(c * CW, CW)]

    def l_quarter(k, q):
        return ll.at[z * (z + 1) // 2 + z - k, col, pl.ds(pl.multiple_of(q * 16, 16), 16)]

    for k in range(4):
        when(root & (z >= k), lambda k=k: pltpu.make_async_copy(
            lp.at[z - k, pl.ds(0, 16)], l_quarter(k, 0), sq.at[k, 0]).start())
    for c in range(8):
        when(root, lambda c=c: pltpu.make_async_copy(
            b.at[pl.ds(0, 128), pl.ds(c * CW, CW)], piece(z, c, 0), gs.at[z, c, 0]).start())
    own_copies = [pltpu.make_async_copy(lp, lo.at[:, col], own_sem)]
    for cp in own_copies:
        cp.start()

    pl.semaphore_wait(barrier, len(around))

    def x_group(ref_of, xs, ts, cond, parity, src=None):
        def j_of(xx, cc):
            return xx * 2 + cc

        def start():
            s = ref_of(col) if src is None else src
            d = ref_of(col)
            put(s, d, xs.at[x], x_dev(1), cond)
            put(s, d, xs.at[x], x_dev(-1), cond)
            put(s, d, ts.at[x], partner, cond)

        def arrive(d, relay):
            xx = (x + d + 4) % 4
            r = ref_of(j_of(xx, core))
            got(r, xs.at[xx], cond)
            if relay:
                put(r, r, xs.at[xx], x_dev(-d), cond)
            put(r, r, ts.at[xx], partner, cond)

        def done():
            for xx in range(4):
                got(ref_of(j_of(xx, 1 - core)), ts.at[xx], cond)

        return start, arrive, done

    for k in range(4):
        conds = [None if k == 0 else blk >= k for blk in blocks]
        groups = [
            x_group(lambda j, blk=blocks[w], k=k: l_ref(blk, k, j), sx.at[blocks[w], k], st.at[blocks[w], k],
                    conds[w], (k + w) % 2)
            for w in range(4)
        ]

        def l_scatter(k=k, cond=conds[OWN]):
            for q in (1, 3, 2):
                put(lp.at[z - k, pl.ds(q * 16, 16)], l_quarter(k, q), sq.at[k, q], y_dev(q),
                    root if cond is None else root & cond)

        def l_mine(k=k, cond=conds[OWN]):
            r, sem = l_quarter(k, y), sq.at[k, y]
            got(r, sem, cond)
            put(r, r, sem, y_dev(1), cond)
            put(r, r, sem, y_dev(-1), cond)

        def l_relay(d, k=k, cond=conds[OWN]):
            q = (y + d + 4) % 4
            r, sem = l_quarter(k, q), sq.at[k, q]
            got(r, sem, cond)
            if d == (-1 if k % 2 == 0 else 1):
                put(r, r, sem, y_dev(-d), cond)

        def l_own(k=k, cond=conds[OWN], start=groups[OWN][0]):
            q = (y + 2) % 4
            got(l_quarter(k, q), sq.at[k, q], cond)
            r, sem = l_ref(z, k), sl.at[z, k]
            put(r, r, sem, z_dev(1), cond)
            put(r, r, sem, z_dev(-1), cond)
            start()

        def l_arrive(w, k=k, conds=conds, groups=groups):
            blk, cond = blocks[w], conds[w]
            r, sem = l_ref(blk, k), sl.at[blk, k]
            got(r, sem, cond)
            if w == (LEFT if k % 2 == 0 else RIGHT):
                put(r, r, sem, z_dev(1 if w == LEFT else -1), cond)
            groups[w][0]()

        task(l_scatter)
        task(l_mine, 30 + k)
        task(functools.partial(l_relay, -1), 30 + k)
        task(functools.partial(l_relay, 1), 30 + k)
        task(l_own, k, (30 + k,))
        for w in (LEFT, RIGHT, OPP):
            task(functools.partial(l_arrive, w), k)
        for w in range(4):
            for d in (-1, 1, 2):
                task(functools.partial(groups[w][1], d, d == (-1 if (k + w) % 2 == 0 else 1)), k)
        for w in range(4):
            task(groups[w][2], k)
    for h in range(4):
        start, arrive, done = x_group(lambda j, h=h: lo.at[h, j], ox.at[h], ot.at[h], None, h % 2, src=lp.at[h])
        task(start)
        for d in (-1, 1, 2):
            task(functools.partial(arrive, d, d == (-1 if h % 2 == 0 else 1)))
        last(done)

    for c in range(8):
        def scatter(c=c):
            for q in (1, 3, 2):
                put(b.at[pl.ds(q * 128, 128), pl.ds(c * CW, CW)], piece(z, c, q), gs.at[z, c, q], y_dev(q), root)

        zfirst = c in Z_FIRST
        pos1, pos2 = (z, y) if zfirst else (y, z)
        dev1, dev2 = (z_dev, y_dev) if zfirst else (y_dev, z_dev)

        def at(e, d, c=c, pos1=pos1, pos2=pos2, zfirst=zfirst):
            i1, i2 = (pos1 + e + 4) % 4, (pos2 + d + 4) % 4
            blk, q = (i1, i2) if zfirst else (i2, i1)
            return piece(blk, c, q), gs.at[blk, c, q]

        def first(e, c=c, at=at, dev1=dev1, dev2=dev2):
            r, sem = at(e, 0)
            got(r, sem)
            if e == 0:
                put(r, r, sem, dev1(1))
                put(r, r, sem, dev1(-1))
            elif e == (-1 if c // 2 % 2 == 0 else 1):
                put(r, r, sem, dev1(-e))
            put(r, r, sem, dev2(1))
            put(r, r, sem, dev2(-1))

        def second(e, d, at=at, dev2=dev2):
            r, sem = at(e, d)
            got(r, sem)
            if d == (-1 if e in (0, 2) else 1):
                put(r, r, sem, dev2(-d))

        task(scatter)
        for e in (0, -1, 1, 2):
            task(functools.partial(first, e), 40 + c // 4)
        for e in (0, -1, 1, 2):
            for d in (-1, 1):
                task(functools.partial(second, e, d), 40 + c // 4)
        for e in (0, -1, 1, 2):
            task(functools.partial(second, e, 2), 40 + c // 4)

    task(lambda: do_inverse(ll, vh, vw), 50, (0,))
    for k in range(1, 4):
        task(functools.partial(do_prep, k, ll, sh, sw), 51, (k,))
    for h in range(2):
        cols = pl.ds(h * HALF, HALF)
        out = pltpu.make_async_copy(xb.at[:, :, cols], x_out.at[:, :, cols], osem.at[h])
        for s in range(4):
            task(functools.partial(do_diag, s, h, g, xb, vh, vw, xh, xl), 60 + 4 * h + s, (50, 40 + h, 69 + 4 * h + s))
            if s < 3:
                task(functools.partial(do_stack, s, h, g, xb, sh, sw, xh, xl), 70 + 4 * h + s, (51, 60 + 4 * h + s))
        task(out.start, None, (63 + 4 * h,))
        last(out.wait)

    for i in arrange(meta, TIMES):
        ops[i]()
    for fn in ends:
        fn()
    for cond, make in sends:
        when(cond, lambda make=make: make().wait_send())
    for cp in own_copies:
        cp.wait()


def dot(a, b):
    return jnp.dot(a, b, preferred_element_type=F32)


def split(v):
    hi = v.astype(BF16)
    return hi, (v - hi.astype(F32)).astype(BF16)


def dot_small(a, b):
    bb = jnp.concatenate(split(b), axis=1)
    r = dot(jnp.concatenate(split(a), axis=1), jnp.concatenate([bb, bb], axis=0))
    return r[:, :128] + r[:, 128:]


def dot3(a, b):
    (ah, al), (bh, bl) = split(a), split(b)
    return dot(ah, bh) + (dot(ah, bl) + dot(al, bh))


def invert_tiles(tiles):
    n = 128
    ri = lax.broadcasted_iota(jnp.int32, (n, n), 0)
    ci = lax.broadcasted_iota(jnp.int32, (n, n), 1)
    eye = ri == ci
    ident = jnp.where(eye, F32(1.0), F32(0.0))
    count = len(tiles)
    scaled, inv_row, parts = [], [], []
    for t in tiles:
        cols, rows = [], []
        for d in range(4):
            blk = t[d * n:(d + 1) * n, d * n:(d + 1) * n]
            diag = jnp.where(eye, blk, F32(0.0))
            cols.append(F32(1.0) / jnp.sum(diag, axis=1, keepdims=True))
            rows.append(F32(1.0) / jnp.sum(diag, axis=0, keepdims=True))
        scaled.append([[t[a * n:(a + 1) * n, c * n:(c + 1) * n] * cols[a] for c in range(a + 1)] for a in range(4)])
        inv_row.append(jnp.concatenate(rows, axis=1))
    for t in scaled:
        for d in range(4):
            parts.append(jnp.where(ri > ci, t[d][d], F32(0.0)))
    same8 = (ri // 8) == (ci // 8)
    small = [jnp.where(same8, p, F32(0.0)) for p in parts]
    sq = [dot_small(m, m) for m in small]
    inv = [(ident - m) for m in small]
    step = [dot_small(v, q) for v, q in zip(inv, sq)]
    quad = [dot_small(q, q) for q in sq]
    inv = [v + s for v, s in zip(inv, step)]
    step = [dot_small(v, q) for v, q in zip(inv, quad)]
    inv = [v + s for v, s in zip(inv, step)]
    for w in (8, 16, 32, 64):
        mask = (ri // (2 * w) == ci // (2 * w)) & ((ri // w) != (ci // w))
        low = [dot_small(jnp.where(mask, p, F32(0.0)), v) for p, v in zip(parts, inv)]
        step = [dot_small(v, s) for v, s in zip(inv, low)]
        inv = [v - s for v, s in zip(inv, step)]
    zero = jnp.zeros((n, n), F32)
    pairs, low = [], []
    for k in range(count):
        for h in range(2):
            low.append(dot_small(scaled[k][2 * h + 1][2 * h], inv[4 * k + 2 * h]))
    for k in range(count):
        for h in range(2):
            a, c = inv[4 * k + 2 * h], inv[4 * k + 2 * h + 1]
            e = -dot_small(c, low[2 * k + h])
            pairs.append(jnp.concatenate(
                [jnp.concatenate([a, zero], axis=1), jnp.concatenate([e, c], axis=1)], axis=0))
    low = []
    for k in range(count):
        t = scaled[k]
        corner = jnp.concatenate(
            [jnp.concatenate(t[2][:2], axis=1), jnp.concatenate(t[3][:2], axis=1)], axis=0)
        low.append(dot3(corner, pairs[2 * k]))
    zero = jnp.zeros((256, 256), F32)
    out = []
    for k in range(count):
        e = -dot3(pairs[2 * k + 1], low[k])
        full = jnp.concatenate(
            [jnp.concatenate([pairs[2 * k], zero], axis=1), jnp.concatenate([e, pairs[2 * k + 1]], axis=1)], axis=0)
        out.append(full * inv_row[k])
    return out


STACK = (0, 1536, 2560, 3072)


def tile_of(ll, r, s):
    return ll[r * (r + 1) // 2 + s].reshape(NB, NB).T


def do_inverse(ll, vh, vw):
    for s, v in enumerate(invert_tiles([tile_of(ll, s, s) for s in range(4)])):
        vh[s], vw[s] = split(v)


def do_prep(k, ll, sh, sw):
    for s in range(4 - k):
        rows = pl.ds(STACK[s] + (k - 1) * NB, NB)
        sh[rows, :], sw[rows, :] = split(tile_of(ll, s + k, s))


def do_diag(s, h, g, xb, vh, vw, xh, xl):
    cols = pl.ds(h * HALF, HALF)
    hi, low = split(g[0, :, cols] if s == 0 else xb[s, :, cols])
    x = dot(vh[s], hi) + (dot(vh[s], low) + dot(vw[s], hi))
    xb[s, :, cols] = x
    xh[h], xl[h] = split(x)


def do_stack(s, h, g, xb, sh, sw, xh, xl):
    cols = pl.ds(h * HALF, HALF)
    rows = pl.ds(STACK[s], STACK[s + 1] - STACK[s])
    upd = dot(sh[rows, :], xh[h]) + (dot(sh[rows, :], xl[h]) + dot(sw[rows, :], xh[h]))
    for r in range(s + 1, 4):
        base = g[r, :, cols] if s == 0 else xb[r, :, cols]
        xb[r, :, cols] = base - upd[(r - s - 1) * NB:(r - s) * NB]


def update_kernel(x, lo, b, x_out, c_out, tiles, oh, ow, sems):
    row = lax.axis_index("row")

    @pl.when(pl.program_id(0) == 0)
    def _():
        copies = [pltpu.make_async_copy(lo.at[s], tiles.at[s], sems.at[s]) for s in range(4)]
        for cp in copies:
            cp.start()
        for s, cp in enumerate(copies):
            cp.wait()
            cols = pl.ds(s * NB, NB)
            oh[:, cols], ow[:, cols] = split(jnp.where(row > s, tiles[s], F32(0.0)).T)

    xs = x[...].reshape(4 * NB, x.shape[2])
    hi, low = split(xs)
    x_out[...] = x[...]
    c_out[...] = b[...] - (dot(oh[...], hi) + (dot(oh[...], low) + dot(ow[...], hi)))


def per_device(lower_panel, right_side):
    lp, b = lower_panel[0], right_side[0]
    width = b.shape[1]
    dma = pltpu.SemaphoreType.DMA
    hbm = pl.BlockSpec(memory_space=pl.ANY)
    vm = pltpu.VMEM
    x, lo = pl.pallas_call(
        gather_kernel,
        out_shape=(jax.ShapeDtypeStruct((4, NB, width), F32), jax.ShapeDtypeStruct((4, 8, 64, NB), F32)),
        in_specs=[hbm, hbm],
        out_specs=(hbm, hbm),
        scratch_shapes=[
            vm((4, NB, width), F32), vm((10, 8, 64, NB), F32), vm((4, NB, width), F32),
            vm((STACK[3], NB), BF16), vm((STACK[3], NB), BF16), vm((4, NB, NB), BF16), vm((4, NB, NB), BF16),
            vm((2, NB, HALF), BF16), vm((2, NB, HALF), BF16),
            dma(()), dma((4, 8, 4)), dma((4, 4)), dma((4, 4)), dma((4, 4, 4)), dma((4, 4, 4)),
            dma((4, 4)), dma((4, 4)), dma((N_SEND,)), dma((2,)),
        ],
        compiler_params=pltpu.CompilerParams(
            collective_id=0, has_side_effects=True, vmem_limit_bytes=66_000_000),
        name="gather",
    )(lp, b)
    lo = lo.reshape(4, NB, NB)
    w = 512
    x, c = pl.pallas_call(
        update_kernel,
        grid=(width // w,),
        out_shape=(jax.ShapeDtypeStruct((4, NB, width), F32), jax.ShapeDtypeStruct((NB, width), F32)),
        in_specs=[
            pl.BlockSpec((4, NB, w), lambda i: (0, 0, i)), hbm, pl.BlockSpec((NB, w), lambda i: (0, i)),
        ],
        out_specs=(pl.BlockSpec((4, NB, w), lambda i: (0, 0, i)), pl.BlockSpec((NB, w), lambda i: (0, i))),
        scratch_shapes=[vm((4, NB, NB), F32), vm((NB, 4 * NB), BF16), vm((NB, 4 * NB), BF16), dma((4,))],
        compiler_params=pltpu.CompilerParams(vmem_limit_bytes=60_000_000),
        name="update",
    )(x, lo, b)
    return x, c[None]


def solution(mesh):
    return jax.shard_map(
        per_device,
        mesh=mesh,
        in_specs=(P(None, None, "col", "row"), P(None, "row", "col")),
        out_specs=(P(None, None, "col"), P(None, "row", "col")),
        check_vma=False,
    )
```

```python
import functools

import jax
import jax.numpy as jnp
from jax import lax
from jax.experimental import pallas as pl
from jax.experimental.pallas import tpu as pltpu
from jax.sharding import PartitionSpec as P

MESH = pl.DeviceIdType.MESH
NB = 512
CW = 128
HALF = 512
Z_FIRST = (1, 3, 5, 7)
Y_PLUS = (0,)
E_PLUS = (0,)
N_SEND = 400
TIMES = (0, 3, 6, 14, 15, 20, 26, 31, 39, 90, 57, 113, 114, 36, 62, 49, 70, 71, 51, 69, 80, 91, 108, 32, 43, 42, 78, 79, 4, 11, 23, 18, 24, 52, 40, 50, 53, 74, 153, 119, 154, 54, 94, 131, 164, 183, 55, 96, 132, 157, 158, 2, 12, 21, 47, 48, 63, 100, 99, 101, 128, 155, 178, 185, 102, 135, 126, 151, 169, 7, 25, 41, 28, 45, 75, 67, 104, 105, 145, 177, 205, 214, 10, 165, 77, 233, 17, 133, 142, 191, 5, 22, 88, 68, 1, 87, 9, 37, 8, 30, 59, 85, 110, 106, 66, 130, 148, 159, 150, 156, 136, 168, 203, 188, 211, 16, 33, 46, 76, 103, 122, 175, 118, 72, 173, 111, 193, 146, 199, 139, 207, 206, 19, 44, 83, 93, 121, 95, 120, 134, 112, 187, 162, 166, 200, 210, 152, 201, 212, 13, 38, 60, 56, 84, 81, 149, 124, 109, 141, 61, 176, 123, 172, 147, 208, 161, 27, 58, 196, 64, 86, 197, 82, 239, 220, 97, 202, 179, 117, 234, 243, 246, 221, 35, 92, 137, 144, 180, 181, 140, 192, 198, 217, 223, 241, 219, 238, 247, 236, 240, 29, 65, 129, 98, 167, 182, 194, 160, 209, 143, 125, 222, 235, 225, 244, 170, 237, 34, 73, 107, 89, 138, 163, 189, 195, 171, 190, 174, 224, 204, 232, 218, 245, 242, 115, 116, 127, 184, 186, 215, 213, 216, 226, 227, 228, 229, 230, 231, 248, 249, 250, 251, 252, 253, 254, 255)
F32, BF16 = jnp.float32, jnp.bfloat16


def when(cond, fn):
    if cond is None:
        fn()
    else:
        pl.when(cond)(fn)


def arrange(meta, times):
    eff = [float(times[i]) if i < len(times) else float(i) for i in range(len(meta))]
    for i, (_, needs) in enumerate(meta):
        for j in range(i):
            if meta[j][0] in needs and eff[j] >= eff[i]:
                eff[i] = eff[j] + 1e-3
    return sorted(range(len(meta)), key=lambda i: (eff[i], i))


def gather_kernel(lp, b, x_out, lo, g, ll, xb, sh, sw, vh, vw, xh, xl, tl, iv, ir, own_sem, gs, sq, sl, sx, st, ox, ot, send, osem):
    row, col = lax.axis_index("row"), lax.axis_index("col")
    y, z = row // 4, row % 4
    x, core = col // 2, col % 2

    def y_dev(d):
        return ((y + d + 4) % 4 * 4 + z, col)

    def z_dev(d):
        return (y * 4 + (z + d + 4) % 4, col)

    def x_dev(d):
        return (row, (x + d + 4) % 4 * 2 + core)

    partner = (row, x * 2 + 1 - core)
    blocks = [(z + d) % 4 for d in (0, 3, 1, 2)]
    OWN, LEFT, RIGHT, OPP = range(4)
    ops, meta, ends, sends = [], [], [], []
    last = ends.append

    def task(fn, tag=None, needs=()):
        ops.append(fn)
        meta.append((tag, needs))

    def put(src, dst, sem, dev, cond=None):
        slot = len(sends)

        def make():
            return pltpu.make_async_remote_copy(
                src_ref=src, dst_ref=dst, send_sem=send.at[slot], recv_sem=sem,
                device_id=dev, device_id_type=MESH,
            )

        sends.append((cond, make))
        when(cond, lambda: make().start())

    def got(ref, sem, cond=None):
        def body():
            pltpu.make_async_copy(ref, ref, sem).wait()

        when(cond, body)

    barrier = pltpu.get_barrier_semaphore()
    around = [y_dev(1), y_dev(-1), y_dev(2), z_dev(1), z_dev(-1), x_dev(1), x_dev(-1), partner]
    for dev in around:
        pl.semaphore_signal(barrier, inc=1, device_id=dev, device_id_type=MESH)

    root, other = y == 0, y != 0

    def l_ref(blk, k, j=None):
        return ll.at[blk * (blk + 1) // 2 + blk - k, col if j is None else j]

    def piece(blk, c, q):
        return g.at[blk, pl.ds(pl.multiple_of(q * 128, 128), 128), pl.ds(c * CW, CW)]

    def l_quarter(k, q):
        return ll.at[z * (z + 1) // 2 + z - k, col, pl.ds(pl.multiple_of(q * 16, 16), 16)]

    for k in range(4):
        when(root & (z >= k), lambda k=k: pltpu.make_async_copy(
            lp.at[z - k, pl.ds(0, 16)], l_quarter(k, 0), sq.at[k, 0]).start())
    for c in range(8):
        when(root, lambda c=c: pltpu.make_async_copy(
            b.at[pl.ds(0, 128), pl.ds(c * CW, CW)], piece(z, c, 0), gs.at[z, c, 0]).start())
    own_copies = [pltpu.make_async_copy(lp, lo.at[:, col], own_sem)]
    for cp in own_copies:
        cp.start()

    pl.semaphore_wait(barrier, len(around))

    def x_group(ref_of, xs, ts, cond, src=None, halved=False):
        def parts(xx, cc, src=None):
            r = ref_of(xx * 2 + cc)
            f = r if src is None else src
            if not halved:
                return [(cond, f, r)]
            low, high = xx < 2, xx >= 2
            if cond is not None:
                low, high = low & cond, high & cond
            tail = pl.ds(NB // 2, NB // 2)
            return [(low, f, r), (high, f.at[:, tail], r.at[:, tail])]

        def start():
            for on, f, r in parts(x, core, src):
                put(f, r, xs.at[x], x_dev(1), on)
                put(f, r, xs.at[x], x_dev(-1), on)
                put(f, r, ts.at[x], partner, on)

        def arrive(d, relay):
            xx = (x + d + 4) % 4
            for on, _, r in parts(xx, core):
                got(r, xs.at[xx], on)
                if relay:
                    put(r, r, xs.at[xx], x_dev(-d), on)
                put(r, r, ts.at[xx], partner, on)

        def done():
            for xx in range(4):
                r, on = ref_of(xx * 2 + 1 - core), cond
                if halved and xx >= 2:
                    r = r.at[:, pl.ds(NB // 2, NB // 2)]
                got(r, ts.at[xx], on)

        return start, arrive, done

    for k in range(4):
        conds = [None if k == 0 else blk >= k for blk in blocks]

        def l_scatter(k=k, cond=conds[OWN]):
            for q in (1, 3, 2):
                put(lp.at[z - k, pl.ds(q * 16, 16)], l_quarter(k, q), sq.at[k, q], y_dev(q),
                    root if cond is None else root & cond)

        def l_mine(k=k, cond=conds[OWN]):
            r, sem = l_quarter(k, y), sq.at[k, y]
            got(r, sem, cond)
            put(r, r, sem, y_dev(1), cond)
            put(r, r, sem, y_dev(-1), cond)

        def l_relay(d, k=k, cond=conds[OWN]):
            q = (y + d + 4) % 4
            r, sem = l_quarter(k, q), sq.at[k, q]
            got(r, sem, cond)
            if d == (-1 if k % 2 == 0 else 1):
                put(r, r, sem, y_dev(-d), cond)

        def l_own(k=k, cond=conds[OWN]):
            q = (y + 2) % 4
            got(l_quarter(k, q), sq.at[k, q], cond)
            r, sem = l_ref(z, k), sl.at[z, k]
            put(r, r, sem, z_dev(1), cond)
            put(r, r, sem, z_dev(-1), cond)

        def l_arrive(w, k=k, conds=conds):
            blk, cond = blocks[w], conds[w]
            r, sem = l_ref(blk, k), sl.at[blk, k]
            got(r, sem, cond)
            if w == (LEFT if k % 2 == 0 else RIGHT):
                put(r, r, sem, z_dev(1 if w == LEFT else -1), cond)

        task(l_scatter)
        task(l_mine, 34 + k)
        task(functools.partial(l_relay, -1), 34 + k)
        task(functools.partial(l_relay, 1), 34 + k)
        task(l_own, 30 + k, (34 + k,))
        for w in (LEFT, RIGHT, OPP):
            task(functools.partial(l_arrive, w), 30 + k)
        for blk in range(k, 4):
            start, arrive, done = x_group(
                lambda j, blk=blk, k=k: l_ref(blk, k, j), sx.at[blk, k], st.at[blk, k], None, None, k == 0)
            unit = 100 + 4 * k + blk
            task(start, unit, (30 + k,))
            for d in (-1, 1, 2):
                task(functools.partial(arrive, d, d == (-1 if (k + blk) % 2 == 0 else 1)), 20 + unit, (unit,))
            task(done, k, (20 + unit,))

    for h in range(4):
        start, arrive, done = x_group(lambda j, h=h: lo.at[h, j], ox.at[h], ot.at[h], None, lp.at[h])
        task(start, 90 + h)
        for d in (-1, 1, 2):
            task(functools.partial(arrive, d, d == (-1 if h % 2 == 0 else 1)), 90 + h)
        last(done)

    for c in range(8):
        def scatter(c=c):
            for q in (1, 3, 2):
                put(b.at[pl.ds(q * 128, 128), pl.ds(c * CW, CW)], piece(z, c, q), gs.at[z, c, q], y_dev(q), root)

        zfirst = c in Z_FIRST
        pos1, pos2 = (z, y) if zfirst else (y, z)
        dev1, dev2 = (z_dev, y_dev) if zfirst else (y_dev, z_dev)

        def at(e, d, c=c, pos1=pos1, pos2=pos2, zfirst=zfirst):
            i1, i2 = (pos1 + e + 4) % 4, (pos2 + d + 4) % 4
            blk, q = (i1, i2) if zfirst else (i2, i1)
            return piece(blk, c, q), gs.at[blk, c, q]

        def first(e, c=c, at=at, dev1=dev1, dev2=dev2, zfirst=zfirst):
            r, sem = at(e, 0)
            got(r, sem)
            if e == 0:
                put(r, r, sem, dev1(1))
                put(r, r, sem, dev1(-1))
            elif e == (-1 if (c // 2 % 2 == 0 if zfirst else c in Y_PLUS) else 1):
                put(r, r, sem, dev1(-e))
            put(r, r, sem, dev2(1))
            put(r, r, sem, dev2(-1))

        def second(e, d, at=at, dev2=dev2, zfirst=zfirst):
            r, sem = at(e, d)
            got(r, sem)
            if d == (-1 if e in (E_PLUS if zfirst else (0, 2)) else 1):
                put(r, r, sem, dev2(-d))

        task(scatter)
        for e in (0, -1, 1, 2):
            task(functools.partial(first, e), 40 + c // 4)
        for e in (0, -1, 1, 2):
            for d in (-1, 1):
                task(functools.partial(second, e, d), 40 + c // 4)
        for e in (0, -1, 1, 2):
            task(functools.partial(second, e, 2), 40 + c // 4)

    task(lambda: do_inverse_base(ll, tl, iv, ir), 48, (0,))
    task(lambda: do_inverse_blocks(tl, iv), 49, (48,))
    task(lambda: do_inverse_join(tl, iv, ir, vh, vw), 50, (49,))
    for k in range(1, 4):
        task(functools.partial(do_prep, k, ll, sh, sw), 51, (k,))
    for h in range(2):
        cols = pl.ds(h * HALF, HALF)
        out = pltpu.make_async_copy(xb.at[:, :, cols], x_out.at[:, :, cols], osem.at[h])
        for s in range(4):
            task(functools.partial(do_diag, s, h, g, xb, vh, vw, xh, xl), 60 + 4 * h + s, (50, 40 + h, 69 + 4 * h + s))
            if s < 3:
                task(functools.partial(do_stack, s, h, g, xb, sh, sw, xh, xl), 70 + 4 * h + s, (51, 60 + 4 * h + s))
        task(out.start, None, (63 + 4 * h,))
        last(out.wait)

    for i in arrange(meta, TIMES):
        ops[i]()
    for fn in ends:
        fn()
    for cond, make in sends:
        when(cond, lambda make=make: make().wait_send())
    for cp in own_copies:
        cp.wait()


def dot(a, b):
    return jnp.dot(a, b, preferred_element_type=F32)


def split(v):
    hi = v.astype(BF16)
    return hi, (v - hi.astype(F32)).astype(BF16)


def dot_small(a, b):
    bb = jnp.concatenate(split(b), axis=1)
    r = dot(jnp.concatenate(split(a), axis=1), jnp.concatenate([bb, bb], axis=0))
    return r[:, :128] + r[:, 128:]


def dot3(a, b):
    (ah, al), (bh, bl) = split(a), split(b)
    return dot(ah, bh) + (dot(ah, bl) + dot(al, bh))


def block_iotas():
    ri = lax.broadcasted_iota(jnp.int32, (CW, CW), 0)
    return ri, lax.broadcasted_iota(jnp.int32, (CW, CW), 1)


def strict_block(tl, i):
    ri, ci = block_iotas()
    rows = pl.ds(i % 4 * CW, CW)
    return jnp.where(ri > ci, tl[i // 4, rows, rows], F32(0.0))


def do_inverse_base(ll, tl, iv, ir):
    ri, ci = block_iotas()
    eye = ri == ci
    for s in range(4):
        t = tile_of(ll, s, s)
        for d in range(4):
            rows = pl.ds(d * CW, CW)
            diag = jnp.where(eye, t[d * CW:(d + 1) * CW, d * CW:(d + 1) * CW], F32(0.0))
            tl[s, rows, :] = t[d * CW:(d + 1) * CW] * (F32(1.0) / jnp.sum(diag, axis=1, keepdims=True))
            ir[s, :, rows] = F32(1.0) / jnp.sum(diag, axis=0, keepdims=True)
    ident = jnp.where(eye, F32(1.0), F32(0.0))
    same8 = (ri // 8) == (ci // 8)
    small = [jnp.where(same8, strict_block(tl, i), F32(0.0)) for i in range(16)]
    sq = [dot_small(m, m) for m in small]
    inv = [(ident - m) for m in small]
    step = [dot_small(v, q) for v, q in zip(inv, sq)]
    quad = [dot_small(q, q) for q in sq]
    inv = [v + s for v, s in zip(inv, step)]
    step = [dot_small(v, q) for v, q in zip(inv, quad)]
    for i in range(16):
        iv[i] = inv[i] + step[i]


def do_inverse_blocks(tl, iv):
    ri, ci = block_iotas()
    inv = [iv[i] for i in range(16)]
    for w in (8, 16, 32, 64):
        mask = (ri // (2 * w) == ci // (2 * w)) & ((ri // w) != (ci // w))
        low = [dot_small(jnp.where(mask, strict_block(tl, i), F32(0.0)), v) for i, v in enumerate(inv)]
        step = [dot_small(v, s) for v, s in zip(inv, low)]
        inv = [v - s for v, s in zip(inv, step)]
    for i in range(16):
        iv[i] = inv[i]


def do_inverse_join(tl, iv, ir, vh, vw):
    zero = jnp.zeros((CW, CW), F32)
    pairs, low = [], []
    for k in range(4):
        for h in range(2):
            rows, cols = pl.ds((2 * h + 1) * CW, CW), pl.ds(2 * h * CW, CW)
            low.append(dot_small(tl[k, rows, cols], iv[4 * k + 2 * h]))
    for k in range(4):
        for h in range(2):
            a, c = iv[4 * k + 2 * h], iv[4 * k + 2 * h + 1]
            e = -dot_small(c, low[2 * k + h])
            pairs.append(jnp.concatenate(
                [jnp.concatenate([a, zero], axis=1), jnp.concatenate([e, c], axis=1)], axis=0))
    low = [dot3(tl[k, pl.ds(256, 256), pl.ds(0, 256)], pairs[2 * k]) for k in range(4)]
    zero = jnp.zeros((256, 256), F32)
    for k in range(4):
        e = -dot3(pairs[2 * k + 1], low[k])
        full = jnp.concatenate(
            [jnp.concatenate([pairs[2 * k], zero], axis=1), jnp.concatenate([e, pairs[2 * k + 1]], axis=1)], axis=0)
        vh[k], vw[k] = split(full * ir[k])


STACK = (0, 1536, 2560, 3072)


def tile_of(ll, r, s):
    return ll[r * (r + 1) // 2 + s].reshape(NB, NB).T


def do_prep(k, ll, sh, sw):
    for s in range(4 - k):
        rows = pl.ds(STACK[s] + (k - 1) * NB, NB)
        sh[rows, :], sw[rows, :] = split(tile_of(ll, s + k, s))


def do_diag(s, h, g, xb, vh, vw, xh, xl):
    cols = pl.ds(h * HALF, HALF)
    hi, low = split(g[0, :, cols] if s == 0 else xb[s, :, cols])
    x = dot(vh[s], hi) + (dot(vh[s], low) + dot(vw[s], hi))
    xb[s, :, cols] = x
    xh[h], xl[h] = split(x)


def do_stack(s, h, g, xb, sh, sw, xh, xl):
    cols = pl.ds(h * HALF, HALF)
    rows = pl.ds(STACK[s], STACK[s + 1] - STACK[s])
    upd = dot(sh[rows, :], xh[h]) + (dot(sh[rows, :], xl[h]) + dot(sw[rows, :], xh[h]))
    for r in range(s + 1, 4):
        base = g[r, :, cols] if s == 0 else xb[r, :, cols]
        xb[r, :, cols] = base - upd[(r - s - 1) * NB:(r - s) * NB]


def update_kernel(x, lo, b, x_out, c_out, tiles, oh, ow, sems):
    row = lax.axis_index("row")

    @pl.when(pl.program_id(0) == 0)
    def _():
        copies = [pltpu.make_async_copy(lo.at[s], tiles.at[s], sems.at[s]) for s in range(4)]
        for cp in copies:
            cp.start()
        for s, cp in enumerate(copies):
            cp.wait()
            cols = pl.ds(s * NB, NB)
            oh[:, cols], ow[:, cols] = split(jnp.where(row > s, tiles[s], F32(0.0)).T)

    xs = x[...].reshape(4 * NB, x.shape[2])
    hi, low = split(xs)
    x_out[...] = x[...]
    c_out[...] = b[...] - (dot(oh[...], hi) + (dot(oh[...], low) + dot(ow[...], hi)))


def per_device(lower_panel, right_side):
    lp, b = lower_panel[0], right_side[0]
    width = b.shape[1]
    dma = pltpu.SemaphoreType.DMA
    hbm = pl.BlockSpec(memory_space=pl.ANY)
    vm = pltpu.VMEM
    x, lo = pl.pallas_call(
        gather_kernel,
        out_shape=(jax.ShapeDtypeStruct((4, NB, width), F32), jax.ShapeDtypeStruct((4, 8, 64, NB), F32)),
        in_specs=[hbm, hbm],
        out_specs=(hbm, hbm),
        scratch_shapes=[
            vm((4, NB, width), F32), vm((10, 8, 64, NB), F32), vm((4, NB, width), F32),
            vm((STACK[3], NB), BF16), vm((STACK[3], NB), BF16), vm((4, NB, NB), BF16), vm((4, NB, NB), BF16),
            vm((2, NB, HALF), BF16), vm((2, NB, HALF), BF16),
            vm((4, NB, NB), F32), vm((16, CW, CW), F32), vm((4, 1, NB), F32),
            dma(()), dma((4, 8, 4)), dma((4, 4)), dma((4, 4)), dma((4, 4, 4)), dma((4, 4, 4)),
            dma((4, 4)), dma((4, 4)), dma((N_SEND,)), dma((2,)),
        ],
        compiler_params=pltpu.CompilerParams(
            collective_id=0, has_side_effects=True, vmem_limit_bytes=66_000_000),
        name="gather",
    )(lp, b)
    lo = lo.reshape(4, NB, NB)
    w = 512
    x, c = pl.pallas_call(
        update_kernel,
        grid=(width // w,),
        out_shape=(jax.ShapeDtypeStruct((4, NB, width), F32), jax.ShapeDtypeStruct((NB, width), F32)),
        in_specs=[
            pl.BlockSpec((4, NB, w), lambda i: (0, 0, i)), hbm, pl.BlockSpec((NB, w), lambda i: (0, i)),
        ],
        out_specs=(pl.BlockSpec((4, NB, w), lambda i: (0, 0, i)), pl.BlockSpec((NB, w), lambda i: (0, i))),
        scratch_shapes=[vm((4, NB, NB), F32), vm((NB, 4 * NB), BF16), vm((NB, 4 * NB), BF16), dma((4,))],
        compiler_params=pltpu.CompilerParams(vmem_limit_bytes=60_000_000),
        name="update",
    )(x, lo, b)
    return x, c[None]


def solution(mesh):
    return jax.shard_map(
        per_device,
        mesh=mesh,
        in_specs=(P(None, None, "col", "row"), P(None, "row", "col")),
        out_specs=(P(None, None, "col"), P(None, "row", "col")),
        check_vma=False,
    )
```

```python
import functools

import jax
import jax.numpy as jnp
from jax import lax
from jax.experimental import pallas as pl
from jax.experimental.pallas import tpu as pltpu
from jax.sharding import PartitionSpec as P

MESH = pl.DeviceIdType.MESH
NB = 512
CW = 128
HALF = 512
Z_FIRST = (1, 3, 5, 7)
Y_PLUS = (0,)
E_PLUS = (0,)
N_SEND = 400
TIMES = (0, 6, 9, 14, 22, 28, 34, 44, 45, 63, 59, 110, 115, 46, 70, 71, 99, 105, 47, 79, 80, 100, 109, 48, 85, 86, 114, 124, 7, 17, 37, 24, 38, 68, 62, 87, 88, 117, 135, 162, 169, 89, 132, 138, 183, 193, 90, 133, 148, 180, 181, 3, 8, 12, 18, 30, 56, 50, 92, 93, 146, 173, 201, 206, 94, 156, 165, 202, 203, 11, 29, 74, 40, 75, 136, 98, 126, 137, 185, 179, 215, 221, 1, 15, 13, 42, 4, 25, 26, 43, 2, 19, 21, 53, 5, 33, 32, 55, 10, 27, 64, 52, 128, 41, 49, 103, 96, 84, 67, 175, 167, 82, 123, 97, 217, 20, 51, 73, 60, 111, 108, 61, 145, 116, 121, 81, 177, 152, 168, 176, 120, 170, 23, 54, 101, 91, 119, 83, 69, 154, 127, 134, 118, 163, 158, 130, 166, 172, 195, 16, 35, 66, 57, 76, 77, 58, 140, 95, 104, 72, 151, 106, 161, 143, 122, 139, 31, 78, 171, 102, 131, 142, 107, 210, 197, 150, 129, 174, 186, 187, 220, 188, 213, 36, 112, 155, 153, 189, 178, 147, 214, 190, 209, 191, 226, 208, 237, 233, 229, 234, 65, 141, 184, 182, 204, 212, 200, 228, 211, 235, 205, 232, 225, 245, 230, 236, 247, 39, 113, 159, 149, 192, 199, 157, 219, 216, 196, 164, 231, 227, 246, 244, 198, 243, 125, 144, 160, 194, 207, 222, 218, 223, 224, 238, 239, 240, 241, 242, 248, 249, 250, 251, 252, 253, 254, 255)
F32, BF16 = jnp.float32, jnp.bfloat16


def when(cond, fn):
    if cond is None:
        fn()
    else:
        pl.when(cond)(fn)


def arrange(meta, times):
    eff = [float(times[i]) if i < len(times) else float(i) for i in range(len(meta))]
    for i, (_, needs) in enumerate(meta):
        for j in range(i):
            if meta[j][0] in needs and eff[j] >= eff[i]:
                eff[i] = eff[j] + 1e-3
    return sorted(range(len(meta)), key=lambda i: (eff[i], i))


def gather_kernel(lp, b, x_out, lo, g, ll, xb, sh, sw, vh, vw, xh, xl, tl, iv, ir, own_sem, gs, sq, sl, sx, st, ox, ot, send, osem):
    row, col = lax.axis_index("row"), lax.axis_index("col")
    y, z = row // 4, row % 4
    x, core = col // 2, col % 2

    def y_dev(d):
        return ((y + d + 4) % 4 * 4 + z, col)

    def z_dev(d):
        return (y * 4 + (z + d + 4) % 4, col)

    def x_dev(d):
        return (row, (x + d + 4) % 4 * 2 + core)

    partner = (row, x * 2 + 1 - core)
    blocks = [(z + d) % 4 for d in (0, 3, 1, 2)]
    OWN, LEFT, RIGHT, OPP = range(4)
    ops, meta, ends, sends = [], [], [], []
    last = ends.append

    def task(fn, tag=None, needs=()):
        ops.append(fn)
        meta.append((tag, needs))

    def put(src, dst, sem, dev, cond=None):
        slot = len(sends)

        def make():
            return pltpu.make_async_remote_copy(
                src_ref=src, dst_ref=dst, send_sem=send.at[slot], recv_sem=sem,
                device_id=dev, device_id_type=MESH,
            )

        sends.append((cond, make))
        when(cond, lambda: make().start())

    def got(ref, sem, cond=None):
        def body():
            pltpu.make_async_copy(ref, ref, sem).wait()

        when(cond, body)

    barrier = pltpu.get_barrier_semaphore()
    around = [y_dev(1), y_dev(-1), y_dev(2), z_dev(1), z_dev(-1), x_dev(1), x_dev(-1), partner]
    for dev in around:
        pl.semaphore_signal(barrier, inc=1, device_id=dev, device_id_type=MESH)

    root, other = y == 0, y != 0

    def l_ref(blk, k, j=None):
        return ll.at[blk * (blk + 1) // 2 + blk - k, col if j is None else j]

    def piece(blk, c, q):
        return g.at[blk, pl.ds(pl.multiple_of(q * 128, 128), 128), pl.ds(c * CW, CW)]

    def l_quarter(k, q):
        return ll.at[z * (z + 1) // 2 + z - k, col, pl.ds(pl.multiple_of(q * 16, 16), 16)]

    for k in range(4):
        when(root & (z >= k), lambda k=k: pltpu.make_async_copy(
            lp.at[z - k, pl.ds(0, 16)], l_quarter(k, 0), sq.at[k, 0]).start())
    for c in range(8):
        when(root, lambda c=c: pltpu.make_async_copy(
            b.at[pl.ds(0, 128), pl.ds(c * CW, CW)], piece(z, c, 0), gs.at[z, c, 0]).start())
    own_copies = [pltpu.make_async_copy(lp, lo.at[:, col], own_sem)]
    for cp in own_copies:
        cp.start()

    pl.semaphore_wait(barrier, len(around))

    def x_group(ref_of, xs, ts, cond, src=None, halved=False):
        def parts(xx, cc, src=None):
            r = ref_of(xx * 2 + cc)
            f = r if src is None else src
            if not halved:
                return [(cond, f, r)]
            low, high = xx < 2, xx >= 2
            if cond is not None:
                low, high = low & cond, high & cond
            tail = pl.ds(NB // 2, NB // 2)
            return [(low, f, r), (high, f.at[:, tail], r.at[:, tail])]

        def start():
            for on, f, r in parts(x, core, src):
                put(f, r, xs.at[x], x_dev(1), on)
                put(f, r, xs.at[x], x_dev(-1), on)
                put(f, r, ts.at[x], partner, on)

        def arrive(d, relay):
            xx = (x + d + 4) % 4
            for on, _, r in parts(xx, core):
                got(r, xs.at[xx], on)
                if relay:
                    put(r, r, xs.at[xx], x_dev(-d), on)
                put(r, r, ts.at[xx], partner, on)

        def done():
            for xx in range(4):
                r, on = ref_of(xx * 2 + 1 - core), cond
                if halved and xx >= 2:
                    r = r.at[:, pl.ds(NB // 2, NB // 2)]
                got(r, ts.at[xx], on)

        return start, arrive, done

    for k in range(4):
        conds = [None if k == 0 else blk >= k for blk in blocks]

        def l_scatter(k=k, cond=conds[OWN]):
            for q in (1, 3, 2):
                put(lp.at[z - k, pl.ds(q * 16, 16)], l_quarter(k, q), sq.at[k, q], y_dev(q),
                    root if cond is None else root & cond)

        def l_mine(k=k, cond=conds[OWN]):
            r, sem = l_quarter(k, y), sq.at[k, y]
            got(r, sem, cond)
            put(r, r, sem, y_dev(1), cond)
            put(r, r, sem, y_dev(-1), cond)

        def l_relay(d, k=k, cond=conds[OWN]):
            q = (y + d + 4) % 4
            r, sem = l_quarter(k, q), sq.at[k, q]
            got(r, sem, cond)
            if d == (-1 if k % 2 == 0 else 1):
                put(r, r, sem, y_dev(-d), cond)

        def l_own(k=k, cond=conds[OWN]):
            q = (y + 2) % 4
            got(l_quarter(k, q), sq.at[k, q], cond)
            r, sem = l_ref(z, k), sl.at[z, k]
            put(r, r, sem, z_dev(1), cond)
            put(r, r, sem, z_dev(-1), cond)

        def l_arrive(w, k=k, conds=conds):
            blk, cond = blocks[w], conds[w]
            r, sem = l_ref(blk, k), sl.at[blk, k]
            got(r, sem, cond)
            if w == (LEFT if k % 2 == 0 else RIGHT):
                put(r, r, sem, z_dev(1 if w == LEFT else -1), cond)

        task(l_scatter)
        task(l_mine, 34 + k)
        task(functools.partial(l_relay, -1), 34 + k)
        task(functools.partial(l_relay, 1), 34 + k)
        task(l_own, 30 + k, (34 + k,))
        for w in (LEFT, RIGHT, OPP):
            task(functools.partial(l_arrive, w), 30 + k)
        for blk in range(k, 4):
            start, arrive, done = x_group(
                lambda j, blk=blk, k=k: l_ref(blk, k, j), sx.at[blk, k], st.at[blk, k], None, None, k == 0)
            unit = 100 + 4 * k + blk
            task(start, unit, (30 + k,))
            for d in (-1, 1, 2):
                task(functools.partial(arrive, d, d == (-1 if (k + blk) % 2 == 0 else 1)), 20 + unit, (unit,))
            task(done, k, (20 + unit,))

    for h in range(4):
        start, arrive, done = x_group(lambda j, h=h: lo.at[h, j], ox.at[h], ot.at[h], None, lp.at[h])
        task(start, 90 + h)
        for d in (-1, 1, 2):
            task(functools.partial(arrive, d, d == (-1 if h % 2 == 0 else 1)), 90 + h)
        last(done)

    for c in range(8):
        def scatter(c=c):
            for q in (1, 3, 2):
                put(b.at[pl.ds(q * 128, 128), pl.ds(c * CW, CW)], piece(z, c, q), gs.at[z, c, q], y_dev(q), root)

        zfirst = c in Z_FIRST
        pos1, pos2 = (z, y) if zfirst else (y, z)
        dev1, dev2 = (z_dev, y_dev) if zfirst else (y_dev, z_dev)

        def at(e, d, c=c, pos1=pos1, pos2=pos2, zfirst=zfirst):
            i1, i2 = (pos1 + e + 4) % 4, (pos2 + d + 4) % 4
            blk, q = (i1, i2) if zfirst else (i2, i1)
            return piece(blk, c, q), gs.at[blk, c, q]

        def first(e, c=c, at=at, dev1=dev1, dev2=dev2, zfirst=zfirst):
            r, sem = at(e, 0)
            got(r, sem)
            if e == 0:
                put(r, r, sem, dev1(1))
                put(r, r, sem, dev1(-1))
            elif e == (-1 if (c // 2 % 2 == 0 if zfirst else c in Y_PLUS) else 1):
                put(r, r, sem, dev1(-e))
            put(r, r, sem, dev2(1))
            put(r, r, sem, dev2(-1))

        def second(e, d, at=at, dev2=dev2, zfirst=zfirst):
            r, sem = at(e, d)
            got(r, sem)
            if d == (-1 if e in (E_PLUS if zfirst else (0, 2)) else 1):
                put(r, r, sem, dev2(-d))

        task(scatter)
        for e in (0, -1, 1, 2):
            task(functools.partial(first, e), 40 + c // 4)
        for e in (0, -1, 1, 2):
            for d in (-1, 1):
                task(functools.partial(second, e, d), 40 + c // 4)
        for e in (0, -1, 1, 2):
            task(functools.partial(second, e, 2), 40 + c // 4)

    task(lambda: do_inverse_base(ll, tl, iv, ir), 48, (0,))
    task(lambda: do_inverse_blocks(tl, iv), 49, (48,))
    task(lambda: do_inverse_join(tl, iv, ir, vh, vw), 50, (49,))
    for k in range(1, 4):
        task(functools.partial(do_prep, k, ll, sh, sw), 51, (k,))
    for h in range(2):
        cols = pl.ds(h * HALF, HALF)
        out = pltpu.make_async_copy(xb.at[:, :, cols], x_out.at[:, :, cols], osem.at[h])
        for s in range(4):
            task(functools.partial(do_diag, s, h, g, xb, vh, vw, xh, xl), 60 + 4 * h + s, (50, 40 + h, 69 + 4 * h + s))
            if s < 3:
                task(functools.partial(do_stack, s, h, g, xb, sh, sw, xh, xl), 70 + 4 * h + s, (51, 60 + 4 * h + s))
        task(out.start, None, (63 + 4 * h,))
        last(out.wait)

    for i in arrange(meta, TIMES):
        ops[i]()
    for fn in ends:
        fn()
    for cond, make in sends:
        when(cond, lambda make=make: make().wait_send())
    for cp in own_copies:
        cp.wait()


def dot(a, b):
    return jnp.dot(a, b, preferred_element_type=F32)


def split(v):
    hi = v.astype(BF16)
    return hi, (v - hi.astype(F32)).astype(BF16)


def dot_small(a, b):
    bb = jnp.concatenate(split(b), axis=1)
    r = dot(jnp.concatenate(split(a), axis=1), jnp.concatenate([bb, bb], axis=0))
    return r[:, :128] + r[:, 128:]


def dot3(a, b):
    (ah, al), (bh, bl) = split(a), split(b)
    return dot(ah, bh) + (dot(ah, bl) + dot(al, bh))


def block_iotas():
    ri = lax.broadcasted_iota(jnp.int32, (CW, CW), 0)
    return ri, lax.broadcasted_iota(jnp.int32, (CW, CW), 1)


def strict_block(tl, i):
    ri, ci = block_iotas()
    rows = pl.ds(i % 4 * CW, CW)
    return jnp.where(ri > ci, tl[i // 4, rows, rows], F32(0.0))


def do_inverse_base(ll, tl, iv, ir):
    ri, ci = block_iotas()
    eye = ri == ci
    for s in range(4):
        t = tile_of(ll, s, s)
        for d in range(4):
            rows = pl.ds(d * CW, CW)
            diag = jnp.where(eye, t[d * CW:(d + 1) * CW, d * CW:(d + 1) * CW], F32(0.0))
            tl[s, rows, :] = t[d * CW:(d + 1) * CW] * (F32(1.0) / jnp.sum(diag, axis=1, keepdims=True))
            ir[s, :, rows] = F32(1.0) / jnp.sum(diag, axis=0, keepdims=True)
    ident = jnp.where(eye, F32(1.0), F32(0.0))
    same8 = (ri // 8) == (ci // 8)
    small = [jnp.where(same8, strict_block(tl, i), F32(0.0)) for i in range(16)]
    sq = [dot_small(m, m) for m in small]
    inv = [(ident - m) for m in small]
    step = [dot_small(v, q) for v, q in zip(inv, sq)]
    quad = [dot_small(q, q) for q in sq]
    inv = [v + s for v, s in zip(inv, step)]
    step = [dot_small(v, q) for v, q in zip(inv, quad)]
    for i in range(16):
        iv[i] = inv[i] + step[i]


def do_inverse_blocks(tl, iv):
    ri, ci = block_iotas()
    inv = [iv[i] for i in range(16)]
    for w in (8, 16, 32, 64):
        mask = (ri // (2 * w) == ci // (2 * w)) & ((ri // w) != (ci // w))
        low = [dot_small(jnp.where(mask, strict_block(tl, i), F32(0.0)), v) for i, v in enumerate(inv)]
        step = [dot_small(v, s) for v, s in zip(inv, low)]
        inv = [v - s for v, s in zip(inv, step)]
    for i in range(16):
        iv[i] = inv[i]


def do_inverse_join(tl, iv, ir, vh, vw):
    zero = jnp.zeros((CW, CW), F32)
    pairs, low = [], []
    for k in range(4):
        for h in range(2):
            rows, cols = pl.ds((2 * h + 1) * CW, CW), pl.ds(2 * h * CW, CW)
            low.append(dot_small(tl[k, rows, cols], iv[4 * k + 2 * h]))
    for k in range(4):
        for h in range(2):
            a, c = iv[4 * k + 2 * h], iv[4 * k + 2 * h + 1]
            e = -dot_small(c, low[2 * k + h])
            pairs.append(jnp.concatenate(
                [jnp.concatenate([a, zero], axis=1), jnp.concatenate([e, c], axis=1)], axis=0))
    low = [dot3(tl[k, pl.ds(256, 256), pl.ds(0, 256)], pairs[2 * k]) for k in range(4)]
    zero = jnp.zeros((256, 256), F32)
    for k in range(4):
        e = -dot3(pairs[2 * k + 1], low[k])
        full = jnp.concatenate(
            [jnp.concatenate([pairs[2 * k], zero], axis=1), jnp.concatenate([e, pairs[2 * k + 1]], axis=1)], axis=0)
        vh[k], vw[k] = split(full * ir[k])


STACK = (0, 1536, 2560, 3072)


def tile_of(ll, r, s):
    return ll[r * (r + 1) // 2 + s].reshape(NB, NB).T


def do_prep(k, ll, sh, sw):
    for s in range(4 - k):
        rows = pl.ds(STACK[s] + (k - 1) * NB, NB)
        sh[rows, :], sw[rows, :] = split(tile_of(ll, s + k, s))


def do_diag(s, h, g, xb, vh, vw, xh, xl):
    cols = pl.ds(h * HALF, HALF)
    hi, low = split(g[0, :, cols] if s == 0 else xb[s, :, cols])
    x = dot(vh[s], hi) + (dot(vh[s], low) + dot(vw[s], hi))
    xb[s, :, cols] = x
    xh[h], xl[h] = split(x)


def do_stack(s, h, g, xb, sh, sw, xh, xl):
    cols = pl.ds(h * HALF, HALF)
    rows = pl.ds(STACK[s], STACK[s + 1] - STACK[s])
    upd = dot(sh[rows, :], xh[h]) + (dot(sh[rows, :], xl[h]) + dot(sw[rows, :], xh[h]))
    for r in range(s + 1, 4):
        base = g[r, :, cols] if s == 0 else xb[r, :, cols]
        xb[r, :, cols] = base - upd[(r - s - 1) * NB:(r - s) * NB]


def update_kernel(x, lo, b, x_out, c_out, xv, bv, cv, tiles, oh, ow, in_sem, out_sem, lo_sem, b_sem):
    row = lax.axis_index("row")
    halves = [pl.ds(h * HALF, HALF) for h in range(2)]
    loads = [pltpu.make_async_copy(lo.at[s], tiles.at[s], lo_sem.at[s]) for s in range(4)]
    ins = [[pltpu.make_async_copy(x.at[s, :, c], xv.at[h, s], in_sem.at[h, s]) for s in range(4)] for h, c in enumerate(halves)]
    outs = [[pltpu.make_async_copy(xv.at[h, s], x_out.at[s, :, c], out_sem.at[h, s]) for s in range(4)]
            for h, c in enumerate(halves)]
    rhs = [pltpu.make_async_copy(b.at[:, c], bv.at[h], b_sem.at[h]) for h, c in enumerate(halves)]
    res = [pltpu.make_async_copy(cv.at[h], c_out.at[:, c], b_sem.at[2 + h]) for h, c in enumerate(halves)]
    for s in range(4):
        loads[s].start()
        ins[0][s].start()
        if s == 0:
            rhs[0].start()
    for cp in ins[1] + rhs[1:]:
        cp.start()
    for h in range(2):
        for s in range(4):
            cols = pl.ds(s * NB, NB)
            if h == 0:
                loads[s].wait()
                oh[:, cols], ow[:, cols] = split(jnp.where(row > s, tiles[s], F32(0.0)).T)
            ins[h][s].wait()
            outs[h][s].start()
            hi, low = split(xv[h, s])
            upd = dot(oh[:, cols], hi) + (dot(oh[:, cols], low) + dot(ow[:, cols], hi))
            if s == 0:
                rhs[h].wait()
            cv[h] = (bv[h] if s == 0 else cv[h]) - upd
        res[h].start()
    for cp in outs[0] + outs[1] + res:
        cp.wait()


def per_device(lower_panel, right_side):
    lp, b = lower_panel[0], right_side[0]
    width = b.shape[1]
    dma = pltpu.SemaphoreType.DMA
    hbm = pl.BlockSpec(memory_space=pl.ANY)
    vm = pltpu.VMEM
    x, lo = pl.pallas_call(
        gather_kernel,
        out_shape=(jax.ShapeDtypeStruct((4, NB, width), F32), jax.ShapeDtypeStruct((4, 8, 64, NB), F32)),
        in_specs=[hbm, hbm],
        out_specs=(hbm, hbm),
        scratch_shapes=[
            vm((4, NB, width), F32), vm((10, 8, 64, NB), F32), vm((4, NB, width), F32),
            vm((STACK[3], NB), BF16), vm((STACK[3], NB), BF16), vm((4, NB, NB), BF16), vm((4, NB, NB), BF16),
            vm((2, NB, HALF), BF16), vm((2, NB, HALF), BF16),
            vm((4, NB, NB), F32), vm((16, CW, CW), F32), vm((4, 1, NB), F32),
            dma(()), dma((4, 8, 4)), dma((4, 4)), dma((4, 4)), dma((4, 4, 4)), dma((4, 4, 4)),
            dma((4, 4)), dma((4, 4)), dma((N_SEND,)), dma((2,)),
        ],
        compiler_params=pltpu.CompilerParams(
            collective_id=0, has_side_effects=True, vmem_limit_bytes=66_000_000),
        name="gather",
    )(lp, b)
    lo = lo.reshape(4, NB, NB)
    x, c = pl.pallas_call(
        update_kernel,
        out_shape=(jax.ShapeDtypeStruct((4, NB, width), F32), jax.ShapeDtypeStruct((NB, width), F32)),
        in_specs=[hbm, hbm, hbm],
        out_specs=(hbm, hbm),
        scratch_shapes=[
            vm((2, 4, NB, HALF), F32), vm((2, NB, HALF), F32), vm((2, NB, HALF), F32), vm((4, NB, NB), F32),
            vm((NB, 4 * NB), BF16), vm((NB, 4 * NB), BF16),
            dma((2, 4)), dma((2, 4)), dma((4,)), dma((4,)),
        ],
        compiler_params=pltpu.CompilerParams(vmem_limit_bytes=60_000_000),
        name="update",
    )(x, lo, b)
    return x, c[None]


def solution(mesh):
    return jax.shard_map(
        per_device,
        mesh=mesh,
        in_specs=(P(None, None, "col", "row"), P(None, "row", "col")),
        out_specs=(P(None, None, "col"), P(None, "row", "col")),
        check_vma=False,
    )
```

```python
import functools

import jax
import jax.numpy as jnp
from jax import lax
from jax.experimental import pallas as pl
from jax.experimental.pallas import tpu as pltpu
from jax.sharding import PartitionSpec as P

MESH = pl.DeviceIdType.MESH
NB = 512
CW = 128
HALF = 512
Z_FIRST = (1, 3, 5, 7)
Y_PLUS = (0,)
E_PLUS = (0,)
N_SEND = 400
TIMES = (0, 3, 6, 15, 16, 26, 40, 41, 42, 62, 74, 97, 98, 43, 89, 68, 93, 94, 44, 73, 85, 109, 110, 45, 83, 102, 128, 134, 9, 18, 38, 27, 39, 72, 58, 76, 77, 116, 103, 176, 183, 78, 142, 125, 189, 190, 108, 157, 141, 206, 207, 10, 23, 32, 52, 53, 80, 79, 111, 112, 137, 162, 174, 185, 113, 159, 150, 184, 203, 12, 34, 67, 57, 92, 133, 120, 154, 155, 192, 194, 217, 226, 13, 28, 37, 60, 5, 20, 19, 56, 2, 21, 17, 47, 1, 11, 7, 36, 4, 8, 29, 22, 65, 87, 25, 49, 69, 31, 59, 119, 86, 132, 138, 84, 166, 24, 46, 61, 64, 82, 118, 63, 122, 88, 126, 90, 152, 96, 177, 104, 117, 156, 35, 81, 136, 123, 146, 144, 121, 201, 171, 169, 153, 181, 216, 173, 210, 180, 218, 33, 66, 107, 91, 115, 158, 101, 143, 130, 165, 140, 151, 163, 214, 178, 188, 196, 14, 30, 70, 48, 71, 160, 50, 99, 105, 75, 106, 100, 114, 202, 145, 147, 148, 54, 124, 161, 187, 193, 199, 149, 213, 197, 220, 223, 224, 221, 243, 231, 246, 242, 55, 129, 182, 164, 200, 186, 170, 215, 211, 205, 191, 229, 236, 235, 234, 212, 245, 51, 95, 139, 131, 195, 198, 127, 225, 175, 179, 172, 233, 232, 230, 209, 222, 244, 135, 167, 168, 208, 204, 227, 219, 228, 237, 238, 239, 240, 241, 247, 248, 249, 250, 251, 252, 253)
F32, BF16 = jnp.float32, jnp.bfloat16


def when(cond, fn):
    if cond is None:
        fn()
    else:
        pl.when(cond)(fn)


def arrange(meta, times):
    eff = [float(times[i]) if i < len(times) else float(i) for i in range(len(meta))]
    for i, (_, needs) in enumerate(meta):
        for j in range(i):
            if meta[j][0] in needs and eff[j] >= eff[i]:
                eff[i] = eff[j] + 1e-3
    return sorted(range(len(meta)), key=lambda i: (eff[i], i))


def gather_kernel(lp, b, x_out, lo, g, ll, xb, sh, sw, vh, vw, xh, xl, tl, iv, ir, own_sem, gs, sq, sl, sx, st, ox, ot, send, osem):
    row, col = lax.axis_index("row"), lax.axis_index("col")
    y, z = row // 4, row % 4
    x, core = col // 2, col % 2

    def y_dev(d):
        return ((y + d + 4) % 4 * 4 + z, col)

    def z_dev(d):
        return (y * 4 + (z + d + 4) % 4, col)

    def x_dev(d):
        return (row, (x + d + 4) % 4 * 2 + core)

    partner = (row, x * 2 + 1 - core)
    blocks = [(z + d) % 4 for d in (0, 3, 1, 2)]
    OWN, LEFT, RIGHT, OPP = range(4)
    ops, meta, ends, sends = [], [], [], []
    last = ends.append

    def task(fn, tag=None, needs=()):
        ops.append(fn)
        meta.append((tag, needs))

    def put(src, dst, sem, dev, cond=None):
        slot = len(sends)

        def make():
            return pltpu.make_async_remote_copy(
                src_ref=src, dst_ref=dst, send_sem=send.at[slot], recv_sem=sem,
                device_id=dev, device_id_type=MESH,
            )

        sends.append((cond, make))
        when(cond, lambda: make().start())

    def got(ref, sem, cond=None):
        def body():
            pltpu.make_async_copy(ref, ref, sem).wait()

        when(cond, body)

    barrier = pltpu.get_barrier_semaphore()
    around = [y_dev(1), y_dev(-1), y_dev(2), z_dev(1), z_dev(-1), x_dev(1), x_dev(-1), partner]
    for dev in around:
        pl.semaphore_signal(barrier, inc=1, device_id=dev, device_id_type=MESH)

    root, other = y == 0, y != 0

    def l_ref(blk, k, j=None):
        return ll.at[blk * (blk + 1) // 2 + blk - k, col if j is None else j]

    def piece(blk, c, q):
        return g.at[blk, pl.ds(pl.multiple_of(q * 128, 128), 128), pl.ds(c * CW, CW)]

    def l_quarter(k, q):
        return ll.at[z * (z + 1) // 2 + z - k, col, pl.ds(pl.multiple_of(q * 16, 16), 16)]

    for k in range(4):
        when(root & (z >= k), lambda k=k: pltpu.make_async_copy(
            lp.at[z - k, pl.ds(0, 16)], l_quarter(k, 0), sq.at[k, 0]).start())
    for c in range(8):
        when(root, lambda c=c: pltpu.make_async_copy(
            b.at[pl.ds(0, 128), pl.ds(c * CW, CW)], piece(z, c, 0), gs.at[z, c, 0]).start())
    own_copies = [pltpu.make_async_copy(lp, lo.at[:, col], own_sem)]
    for cp in own_copies:
        cp.start()

    pl.semaphore_wait(barrier, len(around))

    def x_group(ref_of, xs, ts, cond, src=None, halved=False):
        def parts(xx, cc, src=None):
            r = ref_of(xx * 2 + cc)
            f = r if src is None else src
            if not halved:
                return [(cond, f, r)]
            low, high = xx < 2, xx >= 2
            if cond is not None:
                low, high = low & cond, high & cond
            tail = pl.ds(NB // 2, NB // 2)
            return [(low, f, r), (high, f.at[:, tail], r.at[:, tail])]

        def start():
            for on, f, r in parts(x, core, src):
                put(f, r, xs.at[x], x_dev(1), on)
                put(f, r, xs.at[x], x_dev(-1), on)
                put(f, r, ts.at[x], partner, on)

        def arrive(d, relay):
            xx = (x + d + 4) % 4
            for on, _, r in parts(xx, core):
                got(r, xs.at[xx], on)
                if relay:
                    put(r, r, xs.at[xx], x_dev(-d), on)
                put(r, r, ts.at[xx], partner, on)

        def done():
            for xx in range(4):
                r, on = ref_of(xx * 2 + 1 - core), cond
                if halved and xx >= 2:
                    r = r.at[:, pl.ds(NB // 2, NB // 2)]
                got(r, ts.at[xx], on)

        return start, arrive, done

    for k in range(4):
        conds = [None if k == 0 else blk >= k for blk in blocks]

        def l_scatter(k=k, cond=conds[OWN]):
            for q in (1, 3, 2):
                put(lp.at[z - k, pl.ds(q * 16, 16)], l_quarter(k, q), sq.at[k, q], y_dev(q),
                    root if cond is None else root & cond)

        def l_mine(k=k, cond=conds[OWN]):
            r, sem = l_quarter(k, y), sq.at[k, y]
            got(r, sem, cond)
            put(r, r, sem, y_dev(1), cond)
            put(r, r, sem, y_dev(-1), cond)

        def l_relay(d, k=k, cond=conds[OWN]):
            q = (y + d + 4) % 4
            r, sem = l_quarter(k, q), sq.at[k, q]
            got(r, sem, cond)
            if d == (-1 if k % 2 == 0 else 1):
                put(r, r, sem, y_dev(-d), cond)

        def l_own(k=k, cond=conds[OWN]):
            q = (y + 2) % 4
            got(l_quarter(k, q), sq.at[k, q], cond)
            r, sem = l_ref(z, k), sl.at[z, k]
            put(r, r, sem, z_dev(1), cond)
            put(r, r, sem, z_dev(-1), cond)

        def l_arrive(w, k=k, conds=conds):
            blk, cond = blocks[w], conds[w]
            r, sem = l_ref(blk, k), sl.at[blk, k]
            got(r, sem, cond)
            if w == (LEFT if k % 2 == 0 else RIGHT):
                put(r, r, sem, z_dev(1 if w == LEFT else -1), cond)

        task(l_scatter)
        task(l_mine, 34 + k)
        task(functools.partial(l_relay, -1), 34 + k)
        task(functools.partial(l_relay, 1), 34 + k)
        task(l_own, 30 + k, (34 + k,))
        for w in (LEFT, RIGHT, OPP):
            task(functools.partial(l_arrive, w), 30 + k)
        for blk in range(k, 4):
            start, arrive, done = x_group(
                lambda j, blk=blk, k=k: l_ref(blk, k, j), sx.at[blk, k], st.at[blk, k], None, None, k == 0)
            unit = 100 + 4 * k + blk
            task(start, unit, (30 + k,))
            for d in (-1, 1, 2):
                task(functools.partial(arrive, d, d == (-1 if (k + blk) % 2 == 0 else 1)), 20 + unit, (unit,))
            task(done, k, (20 + unit,))

    for h in range(4):
        start, arrive, done = x_group(lambda j, h=h: lo.at[h, j], ox.at[h], ot.at[h], None, lp.at[h])
        task(start, 90 + h)
        for d in (-1, 1, 2):
            task(functools.partial(arrive, d, d == (-1 if h % 2 == 0 else 1)), 90 + h)
        last(done)

    for c in range(8):
        def scatter(c=c):
            for q in (1, 3, 2):
                put(b.at[pl.ds(q * 128, 128), pl.ds(c * CW, CW)], piece(z, c, q), gs.at[z, c, q], y_dev(q), root)

        zfirst = c in Z_FIRST
        pos1, pos2 = (z, y) if zfirst else (y, z)
        dev1, dev2 = (z_dev, y_dev) if zfirst else (y_dev, z_dev)

        def at(e, d, c=c, pos1=pos1, pos2=pos2, zfirst=zfirst):
            i1, i2 = (pos1 + e + 4) % 4, (pos2 + d + 4) % 4
            blk, q = (i1, i2) if zfirst else (i2, i1)
            return piece(blk, c, q), gs.at[blk, c, q]

        def first(e, c=c, at=at, dev1=dev1, dev2=dev2, zfirst=zfirst):
            r, sem = at(e, 0)
            got(r, sem)
            if e == 0:
                put(r, r, sem, dev1(1))
                put(r, r, sem, dev1(-1))
            elif e == (-1 if (c // 2 % 2 == 0 if zfirst else c in Y_PLUS) else 1):
                put(r, r, sem, dev1(-e))
            put(r, r, sem, dev2(1))
            put(r, r, sem, dev2(-1))

        def second(e, d, at=at, dev2=dev2, zfirst=zfirst):
            r, sem = at(e, d)
            got(r, sem)
            if d == (-1 if e in (E_PLUS if zfirst else (0, 2)) else 1):
                put(r, r, sem, dev2(-d))

        task(scatter)
        for e in (0, -1, 1, 2):
            task(functools.partial(first, e), 40 + c // 4)
        for e in (0, -1, 1, 2):
            for d in (-1, 1):
                task(functools.partial(second, e, d), 40 + c // 4)
        for e in (0, -1, 1, 2):
            task(functools.partial(second, e, 2), 40 + c // 4)

    task(lambda: do_inverse_base(ll, tl, iv, ir), 48, (0,))
    task(lambda: do_inverse_blocks(tl, iv), 49, (48,))
    task(lambda: do_inverse_join(tl, iv, ir, vh, vw), 50, (49,))
    for k in range(1, 4):
        task(functools.partial(do_prep, k, ll, sh, sw), 51, (k,))
    for h in range(2):
        cols = pl.ds(h * HALF, HALF)
        for s in range(4):
            out = pltpu.make_async_copy(xb.at[s, :, cols], x_out.at[s, :, cols], osem.at[h, s])

            def diag(s=s, h=h, out=out):
                do_diag(s, h, g, xb, vh, vw, xh, xl)
                out.start()

            task(diag, 60 + 4 * h + s, (50, 40 + h, 69 + 4 * h + s))
            last(out.wait)
            if s < 3:
                task(functools.partial(do_stack, s, h, g, xb, sh, sw, xh, xl), 70 + 4 * h + s, (51, 60 + 4 * h + s))

    for i in arrange(meta, TIMES):
        ops[i]()
    for fn in ends:
        fn()
    for cond, make in sends:
        when(cond, lambda make=make: make().wait_send())
    for cp in own_copies:
        cp.wait()


def dot(a, b):
    return jnp.dot(a, b, preferred_element_type=F32)


def split(v):
    hi = v.astype(BF16)
    return hi, (v - hi.astype(F32)).astype(BF16)


def dot_small(a, b):
    bb = jnp.concatenate(split(b), axis=1)
    r = dot(jnp.concatenate(split(a), axis=1), jnp.concatenate([bb, bb], axis=0))
    return r[:, :128] + r[:, 128:]


def dot3(a, b):
    (ah, al), (bh, bl) = split(a), split(b)
    return dot(ah, bh) + (dot(ah, bl) + dot(al, bh))


def block_iotas():
    ri = lax.broadcasted_iota(jnp.int32, (CW, CW), 0)
    return ri, lax.broadcasted_iota(jnp.int32, (CW, CW), 1)


def strict_block(tl, i):
    ri, ci = block_iotas()
    rows = pl.ds(i % 4 * CW, CW)
    return jnp.where(ri > ci, tl[i // 4, rows, rows], F32(0.0))


def do_inverse_base(ll, tl, iv, ir):
    ri, ci = block_iotas()
    eye = ri == ci
    for s in range(4):
        t = tile_of(ll, s, s)
        for d in range(4):
            rows = pl.ds(d * CW, CW)
            diag = jnp.where(eye, t[d * CW:(d + 1) * CW, d * CW:(d + 1) * CW], F32(0.0))
            tl[s, rows, :] = t[d * CW:(d + 1) * CW] * (F32(1.0) / jnp.sum(diag, axis=1, keepdims=True))
            ir[s, :, rows] = F32(1.0) / jnp.sum(diag, axis=0, keepdims=True)
    ident = jnp.where(eye, F32(1.0), F32(0.0))
    same8 = (ri // 8) == (ci // 8)
    small = [jnp.where(same8, strict_block(tl, i), F32(0.0)) for i in range(16)]
    sq = [dot_small(m, m) for m in small]
    inv = [(ident - m) for m in small]
    step = [dot_small(v, q) for v, q in zip(inv, sq)]
    quad = [dot_small(q, q) for q in sq]
    inv = [v + s for v, s in zip(inv, step)]
    step = [dot_small(v, q) for v, q in zip(inv, quad)]
    for i in range(16):
        iv[i] = inv[i] + step[i]


def do_inverse_blocks(tl, iv):
    ri, ci = block_iotas()
    inv = [iv[i] for i in range(16)]
    for w in (8, 16, 32, 64):
        mask = (ri // (2 * w) == ci // (2 * w)) & ((ri // w) != (ci // w))
        low = [dot_small(jnp.where(mask, strict_block(tl, i), F32(0.0)), v) for i, v in enumerate(inv)]
        step = [dot_small(v, s) for v, s in zip(inv, low)]
        inv = [v - s for v, s in zip(inv, step)]
    for i in range(16):
        iv[i] = inv[i]


def do_inverse_join(tl, iv, ir, vh, vw):
    zero = jnp.zeros((CW, CW), F32)
    pairs, low = [], []
    for k in range(4):
        for h in range(2):
            rows, cols = pl.ds((2 * h + 1) * CW, CW), pl.ds(2 * h * CW, CW)
            low.append(dot_small(tl[k, rows, cols], iv[4 * k + 2 * h]))
    for k in range(4):
        for h in range(2):
            a, c = iv[4 * k + 2 * h], iv[4 * k + 2 * h + 1]
            e = -dot_small(c, low[2 * k + h])
            pairs.append(jnp.concatenate(
                [jnp.concatenate([a, zero], axis=1), jnp.concatenate([e, c], axis=1)], axis=0))
    low = [dot3(tl[k, pl.ds(256, 256), pl.ds(0, 256)], pairs[2 * k]) for k in range(4)]
    zero = jnp.zeros((256, 256), F32)
    for k in range(4):
        e = -dot3(pairs[2 * k + 1], low[k])
        full = jnp.concatenate(
            [jnp.concatenate([pairs[2 * k], zero], axis=1), jnp.concatenate([e, pairs[2 * k + 1]], axis=1)], axis=0)
        vh[k], vw[k] = split(full * ir[k])


STACK = (0, 1536, 2560, 3072)


def tile_of(ll, r, s):
    return ll[r * (r + 1) // 2 + s].reshape(NB, NB).T


def do_prep(k, ll, sh, sw):
    for s in range(4 - k):
        rows = pl.ds(STACK[s] + (k - 1) * NB, NB)
        sh[rows, :], sw[rows, :] = split(tile_of(ll, s + k, s))


def do_diag(s, h, g, xb, vh, vw, xh, xl):
    cols = pl.ds(h * HALF, HALF)
    hi, low = split(g[0, :, cols] if s == 0 else xb[s, :, cols])
    half = NB // 2
    a, w = vh[s, :half, :half], vw[s, :half, :half]
    top = dot(a, hi[:half]) + (dot(a, low[:half]) + dot(w, hi[:half]))
    a, w = vh[s, half:, :], vw[s, half:, :]
    x = jnp.concatenate([top, dot(a, hi) + (dot(a, low) + dot(w, hi))], axis=0)
    xb[s, :, cols] = x
    xh[h], xl[h] = split(x)


def do_stack(s, h, g, xb, sh, sw, xh, xl):
    cols = pl.ds(h * HALF, HALF)
    rows = pl.ds(STACK[s], STACK[s + 1] - STACK[s])
    upd = dot(sh[rows, :], xh[h]) + (dot(sh[rows, :], xl[h]) + dot(sw[rows, :], xh[h]))
    for r in range(s + 1, 4):
        base = g[r, :, cols] if s == 0 else xb[r, :, cols]
        xb[r, :, cols] = base - upd[(r - s - 1) * NB:(r - s) * NB]


def update_kernel(x, lo, b, x_out, c_out, xv, bv, cv, tiles, oh, ow, in_sem, out_sem, lo_sem, b_sem):
    row = lax.axis_index("row")
    halves = [pl.ds(h * HALF, HALF) for h in range(2)]
    loads = [pltpu.make_async_copy(lo.at[s], tiles.at[s], lo_sem.at[s]) for s in range(4)]
    ins = [[pltpu.make_async_copy(x.at[s, :, c], xv.at[h, s], in_sem.at[h, s]) for s in range(4)] for h, c in enumerate(halves)]
    outs = [[pltpu.make_async_copy(xv.at[h, s], x_out.at[s, :, c], out_sem.at[h, s]) for s in range(4)]
            for h, c in enumerate(halves)]
    rhs = [pltpu.make_async_copy(b.at[:, c], bv.at[h], b_sem.at[h]) for h, c in enumerate(halves)]
    res = [pltpu.make_async_copy(cv.at[h], c_out.at[:, c], b_sem.at[2 + h]) for h, c in enumerate(halves)]
    for s in range(4):
        loads[s].start()
        ins[0][s].start()
        if s == 0:
            rhs[0].start()
    for cp in ins[1] + rhs[1:]:
        cp.start()
    for h in range(2):
        for s in range(4):
            cols = pl.ds(s * NB, NB)
            if h == 0:
                loads[s].wait()
                oh[:, cols], ow[:, cols] = split(jnp.where(row > s, tiles[s], F32(0.0)).T)
            ins[h][s].wait()
            outs[h][s].start()
            hi, low = split(xv[h, s])
            upd = dot(oh[:, cols], hi) + (dot(oh[:, cols], low) + dot(ow[:, cols], hi))
            if s == 0:
                rhs[h].wait()
            cv[h] = (bv[h] if s == 0 else cv[h]) - upd
        res[h].start()
    for cp in outs[0] + outs[1] + res:
        cp.wait()


def per_device(lower_panel, right_side):
    lp, b = lower_panel[0], right_side[0]
    width = b.shape[1]
    dma = pltpu.SemaphoreType.DMA
    hbm = pl.BlockSpec(memory_space=pl.ANY)
    vm = pltpu.VMEM
    x, lo = pl.pallas_call(
        gather_kernel,
        out_shape=(jax.ShapeDtypeStruct((4, NB, width), F32), jax.ShapeDtypeStruct((4, 8, 64, NB), F32)),
        in_specs=[hbm, hbm],
        out_specs=(hbm, hbm),
        scratch_shapes=[
            vm((4, NB, width), F32), vm((10, 8, 64, NB), F32), vm((4, NB, width), F32),
            vm((STACK[3], NB), BF16), vm((STACK[3], NB), BF16), vm((4, NB, NB), BF16), vm((4, NB, NB), BF16),
            vm((2, NB, HALF), BF16), vm((2, NB, HALF), BF16),
            vm((4, NB, NB), F32), vm((16, CW, CW), F32), vm((4, 1, NB), F32),
            dma(()), dma((4, 8, 4)), dma((4, 4)), dma((4, 4)), dma((4, 4, 4)), dma((4, 4, 4)),
            dma((4, 4)), dma((4, 4)), dma((N_SEND,)), dma((2, 4)),
        ],
        compiler_params=pltpu.CompilerParams(
            collective_id=0, has_side_effects=True, vmem_limit_bytes=66_000_000),
        name="gather",
    )(lp, b)
    lo = lo.reshape(4, NB, NB)
    x, c = pl.pallas_call(
        update_kernel,
        out_shape=(jax.ShapeDtypeStruct((4, NB, width), F32), jax.ShapeDtypeStruct((NB, width), F32)),
        in_specs=[hbm, hbm, hbm],
        out_specs=(hbm, hbm),
        scratch_shapes=[
            vm((2, 4, NB, HALF), F32), vm((2, NB, HALF), F32), vm((2, NB, HALF), F32), vm((4, NB, NB), F32),
            vm((NB, 4 * NB), BF16), vm((NB, 4 * NB), BF16),
            dma((2, 4)), dma((2, 4)), dma((4,)), dma((4,)),
        ],
        compiler_params=pltpu.CompilerParams(vmem_limit_bytes=60_000_000),
        name="update",
    )(x, lo, b)
    return x, c[None]


def solution(mesh):
    return jax.shard_map(
        per_device,
        mesh=mesh,
        in_specs=(P(None, None, "col", "row"), P(None, "row", "col")),
        out_specs=(P(None, None, "col"), P(None, "row", "col")),
        check_vma=False,
    )
```

```python
import functools

import jax
import jax.numpy as jnp
from jax import lax
from jax.experimental import pallas as pl
from jax.experimental.pallas import tpu as pltpu
from jax.sharding import PartitionSpec as P

MESH = pl.DeviceIdType.MESH
NB = 512
CW = 128
HALF = 512
Z_FIRST = (1, 3, 5, 7)
Y_PLUS = (0,)
E_PLUS = (0,)
N_SEND = 400
TIMES = (0, 6, 9, 14, 22, 28, 34, 44, 45, 63, 59, 110, 115, 46, 70, 71, 99, 105, 47, 79, 80, 100, 109, 48, 85, 86, 114, 124, 7, 17, 37, 24, 38, 68, 62, 87, 88, 117, 135, 162, 169, 89, 132, 138, 183, 193, 90, 133, 148, 180, 181, 3, 8, 12, 18, 30, 56, 50, 92, 93, 146, 173, 201, 206, 94, 156, 165, 202, 203, 11, 29, 74, 40, 75, 136, 98, 126, 137, 185, 179, 215, 221, 1, 15, 13, 42, 4, 25, 26, 43, 2, 19, 21, 53, 5, 33, 32, 55, 10, 27, 64, 52, 128, 41, 49, 103, 96, 84, 67, 175, 167, 82, 123, 97, 217, 20, 51, 73, 60, 111, 108, 61, 145, 116, 121, 81, 177, 152, 168, 176, 120, 170, 23, 54, 101, 91, 119, 83, 69, 154, 127, 134, 118, 163, 158, 130, 166, 172, 195, 16, 35, 66, 57, 76, 77, 58, 140, 95, 104, 72, 151, 106, 161, 143, 122, 139, 31, 78, 171, 102, 131, 142, 107, 210, 197, 150, 129, 174, 186, 187, 220, 188, 213, 36, 112, 155, 153, 189, 178, 147, 214, 190, 209, 191, 226, 208, 237, 233, 229, 234, 65, 141, 184, 182, 204, 212, 200, 228, 211, 235, 205, 232, 225, 245, 230, 236, 247, 39, 113, 159, 149, 192, 199, 157, 219, 216, 196, 164, 231, 227, 246, 244, 198, 243, 125, 144, 160, 194, 207, 222, 218, 223, 224, 238, 239, 240, 241, 248, 249, 250, 251, 252, 253, 254)
F32, BF16 = jnp.float32, jnp.bfloat16


def when(cond, fn):
    if cond is None:
        fn()
    else:
        pl.when(cond)(fn)


def arrange(meta, times):
    eff = [float(times[i]) if i < len(times) else float(i) for i in range(len(meta))]
    for i, (_, needs) in enumerate(meta):
        for j in range(i):
            if meta[j][0] in needs and eff[j] >= eff[i]:
                eff[i] = eff[j] + 1e-3
    return sorted(range(len(meta)), key=lambda i: (eff[i], i))


def gather_kernel(lp, b, x_out, lo, g, ll, xb, sh, sw, vh, vw, xh, xl, tl, iv, ir, own_sem, gs, sq, sl, sx, st, ox, ot, send, osem):
    row, col = lax.axis_index("row"), lax.axis_index("col")
    y, z = row // 4, row % 4
    x, core = col // 2, col % 2

    def y_dev(d):
        return ((y + d + 4) % 4 * 4 + z, col)

    def z_dev(d):
        return (y * 4 + (z + d + 4) % 4, col)

    def x_dev(d):
        return (row, (x + d + 4) % 4 * 2 + core)

    partner = (row, x * 2 + 1 - core)
    blocks = [(z + d) % 4 for d in (0, 3, 1, 2)]
    OWN, LEFT, RIGHT, OPP = range(4)
    ops, meta, ends, sends = [], [], [], []
    last = ends.append

    def task(fn, tag=None, needs=()):
        ops.append(fn)
        meta.append((tag, needs))

    def put(src, dst, sem, dev, cond=None):
        slot = len(sends)

        def make():
            return pltpu.make_async_remote_copy(
                src_ref=src, dst_ref=dst, send_sem=send.at[slot], recv_sem=sem,
                device_id=dev, device_id_type=MESH,
            )

        sends.append((cond, make))
        when(cond, lambda: make().start())

    def got(ref, sem, cond=None):
        def body():
            pltpu.make_async_copy(ref, ref, sem).wait()

        when(cond, body)

    barrier = pltpu.get_barrier_semaphore()
    around = [y_dev(1), y_dev(-1), y_dev(2), z_dev(1), z_dev(-1), x_dev(1), x_dev(-1), partner]
    for dev in around:
        pl.semaphore_signal(barrier, inc=1, device_id=dev, device_id_type=MESH)

    root, other = y == 0, y != 0

    def l_ref(blk, k, j=None):
        return ll.at[blk * (blk + 1) // 2 + blk - k, col if j is None else j]

    def piece(blk, c, q):
        return g.at[blk, pl.ds(pl.multiple_of(q * 128, 128), 128), pl.ds(c * CW, CW)]

    def l_quarter(k, q):
        return ll.at[z * (z + 1) // 2 + z - k, col, pl.ds(pl.multiple_of(q * 16, 16), 16)]

    for k in range(4):
        when(root & (z >= k), lambda k=k: pltpu.make_async_copy(
            lp.at[z - k, pl.ds(0, 16)], l_quarter(k, 0), sq.at[k, 0]).start())
    for c in range(8):
        when(root, lambda c=c: pltpu.make_async_copy(
            b.at[pl.ds(0, 128), pl.ds(c * CW, CW)], piece(z, c, 0), gs.at[z, c, 0]).start())
    own_copies = [pltpu.make_async_copy(lp, lo.at[:, col], own_sem)]
    for cp in own_copies:
        cp.start()

    pl.semaphore_wait(barrier, len(around))

    def x_group(ref_of, xs, ts, cond, src=None, halved=False):
        def parts(xx, cc, src=None):
            r = ref_of(xx * 2 + cc)
            f = r if src is None else src
            if not halved:
                return [(cond, f, r)]
            low, high = xx < 2, xx >= 2
            if cond is not None:
                low, high = low & cond, high & cond
            tail = pl.ds(NB // 2, NB // 2)
            return [(low, f, r), (high, f.at[:, tail], r.at[:, tail])]

        def start():
            for on, f, r in parts(x, core, src):
                put(f, r, xs.at[x], x_dev(1), on)
                put(f, r, xs.at[x], x_dev(-1), on)
                put(f, r, ts.at[x], partner, on)

        def arrive(d, relay):
            xx = (x + d + 4) % 4
            for on, _, r in parts(xx, core):
                got(r, xs.at[xx], on)
                if relay:
                    put(r, r, xs.at[xx], x_dev(-d), on)
                put(r, r, ts.at[xx], partner, on)

        def done():
            for xx in range(4):
                r, on = ref_of(xx * 2 + 1 - core), cond
                if halved and xx >= 2:
                    r = r.at[:, pl.ds(NB // 2, NB // 2)]
                got(r, ts.at[xx], on)

        return start, arrive, done

    for k in range(4):
        conds = [None if k == 0 else blk >= k for blk in blocks]

        def l_scatter(k=k, cond=conds[OWN]):
            for q in (1, 3, 2):
                put(lp.at[z - k, pl.ds(q * 16, 16)], l_quarter(k, q), sq.at[k, q], y_dev(q),
                    root if cond is None else root & cond)

        def l_mine(k=k, cond=conds[OWN]):
            r, sem = l_quarter(k, y), sq.at[k, y]
            got(r, sem, cond)
            put(r, r, sem, y_dev(1), cond)
            put(r, r, sem, y_dev(-1), cond)

        def l_relay(d, k=k, cond=conds[OWN]):
            q = (y + d + 4) % 4
            r, sem = l_quarter(k, q), sq.at[k, q]
            got(r, sem, cond)
            if d == (-1 if k % 2 == 0 else 1):
                put(r, r, sem, y_dev(-d), cond)

        def l_own(k=k, cond=conds[OWN]):
            q = (y + 2) % 4
            got(l_quarter(k, q), sq.at[k, q], cond)
            r, sem = l_ref(z, k), sl.at[z, k]
            put(r, r, sem, z_dev(1), cond)
            put(r, r, sem, z_dev(-1), cond)

        def l_arrive(w, k=k, conds=conds):
            blk, cond = blocks[w], conds[w]
            r, sem = l_ref(blk, k), sl.at[blk, k]
            got(r, sem, cond)
            if w == (LEFT if k % 2 == 0 else RIGHT):
                put(r, r, sem, z_dev(1 if w == LEFT else -1), cond)

        task(l_scatter)
        task(l_mine, 34 + k)
        task(functools.partial(l_relay, -1), 34 + k)
        task(functools.partial(l_relay, 1), 34 + k)
        task(l_own, 30 + k, (34 + k,))
        for w in (LEFT, RIGHT, OPP):
            task(functools.partial(l_arrive, w), 30 + k)
        for blk in range(k, 4):
            start, arrive, done = x_group(
                lambda j, blk=blk, k=k: l_ref(blk, k, j), sx.at[blk, k], st.at[blk, k], None, None, k == 0)
            unit = 100 + 4 * k + blk
            task(start, unit, (30 + k,))
            for d in (-1, 1, 2):
                task(functools.partial(arrive, d, d == (-1 if (k + blk) % 2 == 0 else 1)), 20 + unit, (unit,))
            task(done, k, (20 + unit,))

    for h in range(4):
        start, arrive, done = x_group(lambda j, h=h: lo.at[h, j], ox.at[h], ot.at[h], None, lp.at[h])
        task(start, 90 + h)
        for d in (-1, 1, 2):
            task(functools.partial(arrive, d, d == (-1 if h % 2 == 0 else 1)), 90 + h)
        last(done)

    for c in range(8):
        def scatter(c=c):
            for q in (1, 3, 2):
                put(b.at[pl.ds(q * 128, 128), pl.ds(c * CW, CW)], piece(z, c, q), gs.at[z, c, q], y_dev(q), root)

        zfirst = c in Z_FIRST
        pos1, pos2 = (z, y) if zfirst else (y, z)
        dev1, dev2 = (z_dev, y_dev) if zfirst else (y_dev, z_dev)

        def at(e, d, c=c, pos1=pos1, pos2=pos2, zfirst=zfirst):
            i1, i2 = (pos1 + e + 4) % 4, (pos2 + d + 4) % 4
            blk, q = (i1, i2) if zfirst else (i2, i1)
            return piece(blk, c, q), gs.at[blk, c, q]

        def first(e, c=c, at=at, dev1=dev1, dev2=dev2, zfirst=zfirst):
            r, sem = at(e, 0)
            got(r, sem)
            if e == 0:
                put(r, r, sem, dev1(1))
                put(r, r, sem, dev1(-1))
            elif e == (-1 if (c // 2 % 2 == 0 if zfirst else c in Y_PLUS) else 1):
                put(r, r, sem, dev1(-e))
            put(r, r, sem, dev2(1))
            put(r, r, sem, dev2(-1))

        def second(e, d, at=at, dev2=dev2, zfirst=zfirst):
            r, sem = at(e, d)
            got(r, sem)
            if d == (-1 if e in (E_PLUS if zfirst else (0, 2)) else 1):
                put(r, r, sem, dev2(-d))

        task(scatter)
        for e in (0, -1, 1, 2):
            task(functools.partial(first, e), 40 + c // 4)
        for e in (0, -1, 1, 2):
            for d in (-1, 1):
                task(functools.partial(second, e, d), 40 + c // 4)
        for e in (0, -1, 1, 2):
            task(functools.partial(second, e, 2), 40 + c // 4)

    task(lambda: do_inverse_base(ll, tl, iv, ir), 48, (0,))
    task(lambda: do_inverse_blocks(tl, iv), 49, (48,))
    task(lambda: do_inverse_join(tl, iv, ir, vh, vw), 50, (49,))
    for k in range(1, 4):
        task(functools.partial(do_prep, k, ll, sh, sw), 51, (k,))
    for h in range(2):
        cols = pl.ds(h * HALF, HALF)
        for s in range(4):
            out = pltpu.make_async_copy(xb.at[s, :, cols], x_out.at[s, :, cols], osem.at[h, s])

            def diag(s=s, h=h, out=out):
                do_diag(s, h, g, xb, vh, vw, xh, xl)
                out.start()

            task(diag, 60 + 4 * h + s, (50, 40 + h, 69 + 4 * h + s))
            last(out.wait)
            if s < 3:
                task(functools.partial(do_stack, s, h, g, xb, sh, sw, xh, xl), 70 + 4 * h + s, (51, 60 + 4 * h + s))

    for i in arrange(meta, TIMES):
        ops[i]()
    for fn in ends:
        fn()
    for cond, make in sends:
        when(cond, lambda make=make: make().wait_send())
    for cp in own_copies:
        cp.wait()


def dot(a, b):
    return jnp.dot(a, b, preferred_element_type=F32)


def split(v):
    hi = v.astype(BF16)
    return hi, (v - hi.astype(F32)).astype(BF16)


def dot_small(a, b):
    bb = jnp.concatenate(split(b), axis=1)
    r = dot(jnp.concatenate(split(a), axis=1), jnp.concatenate([bb, bb], axis=0))
    return r[:, :128] + r[:, 128:]


def dot3(a, b):
    (ah, al), (bh, bl) = split(a), split(b)
    return dot(ah, bh) + (dot(ah, bl) + dot(al, bh))


def block_iotas():
    ri = lax.broadcasted_iota(jnp.int32, (CW, CW), 0)
    return ri, lax.broadcasted_iota(jnp.int32, (CW, CW), 1)


def strict_block(tl, i):
    ri, ci = block_iotas()
    rows = pl.ds(i % 4 * CW, CW)
    return jnp.where(ri > ci, tl[i // 4, rows, rows], F32(0.0))


def do_inverse_base(ll, tl, iv, ir):
    ri, ci = block_iotas()
    eye = ri == ci
    for s in range(4):
        t = tile_of(ll, s, s)
        for d in range(4):
            rows = pl.ds(d * CW, CW)
            diag = jnp.where(eye, t[d * CW:(d + 1) * CW, d * CW:(d + 1) * CW], F32(0.0))
            tl[s, rows, :] = t[d * CW:(d + 1) * CW] * (F32(1.0) / jnp.sum(diag, axis=1, keepdims=True))
            ir[s, :, rows] = F32(1.0) / jnp.sum(diag, axis=0, keepdims=True)
    ident = jnp.where(eye, F32(1.0), F32(0.0))
    same8 = (ri // 8) == (ci // 8)
    small = [jnp.where(same8, strict_block(tl, i), F32(0.0)) for i in range(16)]
    sq = [dot_small(m, m) for m in small]
    inv = [(ident - m) for m in small]
    step = [dot_small(v, q) for v, q in zip(inv, sq)]
    quad = [dot_small(q, q) for q in sq]
    inv = [v + s for v, s in zip(inv, step)]
    step = [dot_small(v, q) for v, q in zip(inv, quad)]
    for i in range(16):
        iv[i] = inv[i] + step[i]


def do_inverse_blocks(tl, iv):
    ri, ci = block_iotas()
    inv = [iv[i] for i in range(16)]
    for w in (8, 16, 32, 64):
        mask = (ri // (2 * w) == ci // (2 * w)) & ((ri // w) != (ci // w))
        low = [dot_small(jnp.where(mask, strict_block(tl, i), F32(0.0)), v) for i, v in enumerate(inv)]
        step = [dot_small(v, s) for v, s in zip(inv, low)]
        inv = [v - s for v, s in zip(inv, step)]
    for i in range(16):
        iv[i] = inv[i]


def do_inverse_join(tl, iv, ir, vh, vw):
    zero = jnp.zeros((CW, CW), F32)
    pairs, low = [], []
    for k in range(4):
        for h in range(2):
            rows, cols = pl.ds((2 * h + 1) * CW, CW), pl.ds(2 * h * CW, CW)
            low.append(dot_small(tl[k, rows, cols], iv[4 * k + 2 * h]))
    for k in range(4):
        for h in range(2):
            a, c = iv[4 * k + 2 * h], iv[4 * k + 2 * h + 1]
            e = -dot_small(c, low[2 * k + h])
            pairs.append(jnp.concatenate(
                [jnp.concatenate([a, zero], axis=1), jnp.concatenate([e, c], axis=1)], axis=0))
    low = [dot3(tl[k, pl.ds(256, 256), pl.ds(0, 256)], pairs[2 * k]) for k in range(4)]
    zero = jnp.zeros((256, 256), F32)
    for k in range(4):
        e = -dot3(pairs[2 * k + 1], low[k])
        full = jnp.concatenate(
            [jnp.concatenate([pairs[2 * k], zero], axis=1), jnp.concatenate([e, pairs[2 * k + 1]], axis=1)], axis=0)
        vh[k], vw[k] = split(full * ir[k])


STACK = (0, 1536, 2560, 3072)


def tile_of(ll, r, s):
    return ll[r * (r + 1) // 2 + s].reshape(NB, NB).T


def do_prep(k, ll, sh, sw):
    for s in range(4 - k):
        rows = pl.ds(STACK[s] + (k - 1) * NB, NB)
        sh[rows, :], sw[rows, :] = split(tile_of(ll, s + k, s))


def do_diag(s, h, g, xb, vh, vw, xh, xl):
    cols = pl.ds(h * HALF, HALF)
    hi, low = split(g[0, :, cols] if s == 0 else xb[s, :, cols])
    half = NB // 2
    a, w = vh[s, :half, :half], vw[s, :half, :half]
    top = dot(a, hi[:half]) + (dot(a, low[:half]) + dot(w, hi[:half]))
    a, w = vh[s, half:, :], vw[s, half:, :]
    x = jnp.concatenate([top, dot(a, hi) + (dot(a, low) + dot(w, hi))], axis=0)
    xb[s, :, cols] = x
    xh[h], xl[h] = split(x)


def do_stack(s, h, g, xb, sh, sw, xh, xl):
    cols = pl.ds(h * HALF, HALF)
    rows = pl.ds(STACK[s], STACK[s + 1] - STACK[s])
    upd = dot(sh[rows, :], xh[h]) + (dot(sh[rows, :], xl[h]) + dot(sw[rows, :], xh[h]))
    for r in range(s + 1, 4):
        base = g[r, :, cols] if s == 0 else xb[r, :, cols]
        xb[r, :, cols] = base - upd[(r - s - 1) * NB:(r - s) * NB]


def update_kernel(x, lo, b, x_out, c_out, xv, bv, cv, tiles, oh, ow, in_sem, out_sem, lo_sem, b_sem):
    row = lax.axis_index("row")
    halves = [pl.ds(h * HALF, HALF) for h in range(2)]
    loads = [pltpu.make_async_copy(lo.at[s], tiles.at[s], lo_sem.at[s]) for s in range(4)]
    ins = [[pltpu.make_async_copy(x.at[s, :, c], xv.at[h, s], in_sem.at[h, s]) for s in range(4)] for h, c in enumerate(halves)]
    outs = [[pltpu.make_async_copy(xv.at[h, s], x_out.at[s, :, c], out_sem.at[h, s]) for s in range(4)]
            for h, c in enumerate(halves)]
    rhs = [pltpu.make_async_copy(b.at[:, c], bv.at[h], b_sem.at[h]) for h, c in enumerate(halves)]
    res = [pltpu.make_async_copy(cv.at[h], c_out.at[:, c], b_sem.at[2 + h]) for h, c in enumerate(halves)]
    for s in range(4):
        loads[s].start()
        ins[0][s].start()
        if s == 0:
            rhs[0].start()
    for cp in ins[1] + rhs[1:]:
        cp.start()
    for h in range(2):
        for s in range(4):
            cols = pl.ds(s * NB, NB)
            if h == 0:
                loads[s].wait()
                oh[:, cols], ow[:, cols] = split(jnp.where(row > s, tiles[s], F32(0.0)).T)
            ins[h][s].wait()
            outs[h][s].start()
            hi, low = split(xv[h, s])
            upd = dot(oh[:, cols], hi) + (dot(oh[:, cols], low) + dot(ow[:, cols], hi))
            if s == 0:
                rhs[h].wait()
            cv[h] = (bv[h] if s == 0 else cv[h]) - upd
        res[h].start()
    for cp in outs[0] + outs[1] + res:
        cp.wait()


def per_device(lower_panel, right_side):
    lp, b = lower_panel[0], right_side[0]
    width = b.shape[1]
    dma = pltpu.SemaphoreType.DMA
    hbm = pl.BlockSpec(memory_space=pl.ANY)
    vm = pltpu.VMEM
    x, lo = pl.pallas_call(
        gather_kernel,
        out_shape=(jax.ShapeDtypeStruct((4, NB, width), F32), jax.ShapeDtypeStruct((4, 8, 64, NB), F32)),
        in_specs=[hbm, hbm],
        out_specs=(hbm, hbm),
        scratch_shapes=[
            vm((4, NB, width), F32), vm((10, 8, 64, NB), F32), vm((4, NB, width), F32),
            vm((STACK[3], NB), BF16), vm((STACK[3], NB), BF16), vm((4, NB, NB), BF16), vm((4, NB, NB), BF16),
            vm((2, NB, HALF), BF16), vm((2, NB, HALF), BF16),
            vm((4, NB, NB), F32), vm((16, CW, CW), F32), vm((4, 1, NB), F32),
            dma(()), dma((4, 8, 4)), dma((4, 4)), dma((4, 4)), dma((4, 4, 4)), dma((4, 4, 4)),
            dma((4, 4)), dma((4, 4)), dma((N_SEND,)), dma((2, 4)),
        ],
        compiler_params=pltpu.CompilerParams(
            collective_id=0, has_side_effects=True, vmem_limit_bytes=66_000_000),
        name="gather",
    )(lp, b)
    lo = lo.reshape(4, NB, NB)
    x, c = pl.pallas_call(
        update_kernel,
        out_shape=(jax.ShapeDtypeStruct((4, NB, width), F32), jax.ShapeDtypeStruct((NB, width), F32)),
        in_specs=[hbm, hbm, hbm],
        out_specs=(hbm, hbm),
        scratch_shapes=[
            vm((2, 4, NB, HALF), F32), vm((2, NB, HALF), F32), vm((2, NB, HALF), F32), vm((4, NB, NB), F32),
            vm((NB, 4 * NB), BF16), vm((NB, 4 * NB), BF16),
            dma((2, 4)), dma((2, 4)), dma((4,)), dma((4,)),
        ],
        compiler_params=pltpu.CompilerParams(vmem_limit_bytes=60_000_000),
        name="update",
    )(x, lo, b)
    return x, c[None]


def solution(mesh):
    return jax.shard_map(
        per_device,
        mesh=mesh,
        in_specs=(P(None, None, "col", "row"), P(None, "row", "col")),
        out_specs=(P(None, None, "col"), P(None, "row", "col")),
        check_vma=False,
    )
```
